8 devices in a mesh: dp: 1 (over z), tp: 2 (over y), ep: 4 (over x, core).
Axes of the slice: x: 2, y: 2, z: 1, core: 2. Of those that a mesh axis runs over, the one named last changes fastest.
Arguments:
- tokens: bfloat16 [8192, 768], P(('dp', 'ep', 'tp'))
- expert_ids: int32 [8192, 1], P(('dp', 'ep', 'tp'))
- gate_vals: float32 [8192, 1], P(('dp', 'ep', 'tp'))
- w_up: bfloat16 [32, 768, 3072], P('ep', None, 'tp')
- w_down: bfloat16 [32, 3072, 768], P('ep', 'tp')
Outputs:
- output: bfloat16 [8192, 768], P(('dp', 'ep', 'tp'))
All inputs are finite; a program needn't handle non-finite values.
Results may differ from the reference program's by a relative error of at most 0.001.
Values are sent between devices in bfloat16 or wider.
A program may use at most 1 GiB of HBM per device.

```python
import jax
import jax.numpy as jnp
from jax import lax

EXPERTS = 32
TOP_K = 1
HIDDEN = 768
FFN_DIM = 3072
TOK_DEV = 1024
EP_SIZE = 4
TP_SIZE = 2

N_SOURCES = EP_SIZE * TP_SIZE
SLOT_CAP = ((5 * TOK_DEV * TOP_K) // (4 * EXPERTS) + 7) // 8 * 8
N_SLOTS = EXPERTS * SLOT_CAP
N_HOT = max(1, EXPERTS // (8 * TOP_K))
HOT_FILL = SLOT_CAP + SLOT_CAP // 8


def draw_routes(perm_key, order_key, offset_key):
    hot_perm = jax.random.permutation(perm_key, EXPERTS).astype(jnp.int32)
    ranks = jnp.arange(TOK_DEV, dtype=jnp.int32)
    first_rank = jnp.where(ranks < N_HOT * HOT_FILL, ranks // HOT_FILL,
                           N_HOT + (ranks - N_HOT * HOT_FILL) % (EXPERTS - N_HOT))
    orders = jax.vmap(lambda sub_key: jax.random.permutation(sub_key, TOK_DEV))(
        jax.random.split(order_key, N_SOURCES))
    first_choice = hot_perm[first_rank[orders]]
    scores = jax.random.randint(offset_key, (N_SOURCES, TOK_DEV, EXPERTS - 1), 0, 2 ** 20) * (EXPERTS - 1)
    scores = scores + jnp.arange(EXPERTS - 1, dtype=jnp.int32)
    picked = lax.top_k(scores, TOP_K)[1][:, :, :TOP_K - 1] + 1
    others = (first_choice[:, :, None] + picked) % EXPERTS
    routes = jnp.concatenate([first_choice[:, :, None], others], axis=2)
    return routes.reshape(N_SOURCES * TOK_DEV, TOP_K).astype(jnp.int32)


def setup_inputs(seed: int = 0, part: int = 0) -> dict:
    part_keys = jax.random.split(jax.random.fold_in(jax.random.key(seed), part), 5)
    weight_keys = jax.random.split(jax.random.key(seed + 1), 2)
    tokens = jax.random.normal(part_keys[0], (N_SOURCES * TOK_DEV, HIDDEN), jnp.float32).astype(jnp.bfloat16)
    expert_ids = draw_routes(part_keys[1], part_keys[2], part_keys[3])
    gate_vals = jax.random.uniform(part_keys[4], (N_SOURCES * TOK_DEV, TOP_K), jnp.float32, 0.5, 1.0)
    w_up = (jax.random.normal(weight_keys[0], (EXPERTS, HIDDEN, FFN_DIM), jnp.float32) * HIDDEN ** -0.5).astype(jnp.bfloat16)
    w_down = (jax.random.normal(weight_keys[1], (EXPERTS, FFN_DIM, HIDDEN), jnp.float32) * FFN_DIM ** -0.5).astype(jnp.bfloat16)
    return {'tokens': tokens, 'expert_ids': expert_ids, 'gate_vals': gate_vals, 'w_up': w_up, 'w_down': w_down}


def slot_table(route_ids):
    expert_hit = (route_ids[:, :, None] == jnp.arange(EXPERTS, dtype=jnp.int32)).astype(jnp.int32)
    chosen = jnp.sum(expert_hit, axis=1)
    prior_count = jnp.cumsum(chosen, axis=0) - chosen
    token_rank = jnp.sum(expert_hit * prior_count[:, None, :], axis=2)
    return jnp.where(token_rank < SLOT_CAP, route_ids * SLOT_CAP + token_rank, -1)


def reference(tokens, expert_ids, gate_vals, w_up, w_down):
    src_rows = tokens.reshape(N_SOURCES, TOK_DEV, HIDDEN)
    src_slots = jax.vmap(slot_table)(expert_ids.reshape(N_SOURCES, TOK_DEV, TOP_K))
    src_gates = gate_vals.reshape(N_SOURCES, TOK_DEV, TOP_K)
    slot_iota = jnp.arange(N_SLOTS, dtype=jnp.int32)

    def dispatch(operands):
        rows_in, slot_ids = operands
        pick_mat = jnp.zeros((N_SLOTS, TOK_DEV), jnp.bfloat16)
        for choice_idx in range(TOP_K):
            pick_mat = pick_mat + (slot_iota[:, None] == slot_ids[None, :, choice_idx]).astype(jnp.bfloat16)
        return jnp.dot(pick_mat, rows_in, preferred_element_type=jnp.float32).astype(jnp.bfloat16)

    buffers = lax.map(dispatch, (src_rows, src_slots))
    per_expert = jnp.transpose(buffers.reshape(N_SOURCES, EXPERTS, SLOT_CAP, HIDDEN), (1, 0, 2, 3))
    per_expert = per_expert.reshape(EXPERTS, N_SOURCES * SLOT_CAP, HIDDEN)

    def expert_ffn(operands):
        rows_in, up_mat, down_mat = operands
        pre_act = jnp.dot(rows_in, up_mat, preferred_element_type=jnp.float32)
        hidden_act = jax.nn.gelu(pre_act, approximate=True).astype(jnp.bfloat16)
        return jnp.dot(hidden_act, down_mat, preferred_element_type=jnp.float32).astype(jnp.bfloat16)

    expert_out = lax.map(expert_ffn, (per_expert, w_up, w_down))
    slot_out = jnp.transpose(expert_out.reshape(EXPERTS, N_SOURCES, SLOT_CAP, HIDDEN), (1, 0, 2, 3))
    slot_out = slot_out.reshape(N_SOURCES, N_SLOTS, HIDDEN)

    def combine(operands):
        results, slot_ids, gate_rows = operands
        gate_sum = jnp.zeros((TOK_DEV, HIDDEN), jnp.float32)
        for choice_idx in range(TOP_K):
            pick_mat = (slot_ids[:, choice_idx, None] == slot_iota[None, :]).astype(jnp.bfloat16)
            picked = jnp.dot(pick_mat, results, preferred_element_type=jnp.float32)
            gate_sum = gate_sum + gate_rows[:, choice_idx, None] * picked
        return gate_sum.astype(jnp.bfloat16)

    moe_out = lax.map(combine, (slot_out, src_slots, src_gates))
    return moe_out.reshape(N_SOURCES * TOK_DEV, HIDDEN)
```

```python
import functools

import jax
import jax.numpy as jnp
from jax import lax
from jax.experimental import pallas as pl
from jax.experimental.pallas import tpu as pltpu
from jax.sharding import PartitionSpec as P

MESH = pl.DeviceIdType.MESH
W_SLOTS = 3


def capacity(tok_count, n_top, n_exp):
    return ((5 * tok_count * n_top) // (4 * n_exp) + 7) // 8 * 8


def moe_kernel(dims, tok_hbm, ids_ref, up_hbm, down_hbm, out_ref,
               tok_own, tok_peer, ids_peer, slot_own, slot_peer, slot_col,
               send_rows, rows, up_buf, down_buf, hid, mine, other, arrived, ret_send, ret_recv,
               tok_sem, w_sem, ids_ss, ids_rs, ytok_ss, ytok_rs, disp_ss, disp_rs,
               part_ss, part_rs, ret_ss, ret_rs, go_sem):
    n_tok, hidden, ffn, n_loc, cap, pad = dims
    n_exp = 4 * n_loc
    f32, bf16 = jnp.float32, jnp.bfloat16
    dp, tp, ep = lax.axis_index('dp'), lax.axis_index('tp'), lax.axis_index('ep')
    core = lax.rem(ep, 2)

    def rel_ep(d):
        flipped = lax.rem(ep + 2 * (d // 2), 4)
        return flipped + (d % 2) * (1 - 2 * lax.rem(flipped, 2))

    def dev(d):
        return (dp, tp, rel_ep(d))

    peer = (dp, 1 - tp, ep)
    partner = dev(1)

    def w_copies(n):
        slot, e = lax.rem(n, W_SLOTS), lax.rem(n, n_loc)
        return (pltpu.make_async_copy(up_hbm.at[e], up_buf.at[slot], w_sem.at[slot, 0]),
                pltpu.make_async_copy(down_hbm.at[e], down_buf.at[slot], w_sem.at[slot, 1]))

    def w_start(n):
        for cp in w_copies(n):
            cp.start()

    tok_cp = pltpu.make_async_copy(tok_hbm, tok_own, tok_sem)
    tok_cp.start()

    barrier = pltpu.get_barrier_semaphore()
    for target in (peer, dev(1), dev(2), dev(3)):
        pl.semaphore_signal(barrier, inc=1, device_id=target, device_id_type=MESH)
    pl.semaphore_wait(barrier, 4)

    ids_cp = pltpu.make_async_remote_copy(ids_ref, ids_peer, ids_ss, ids_rs, device_id=peer, device_id_type=MESH)
    ids_cp.start()
    tok_cp.wait()

    cut = n_tok * 7 // 8
    ytok = [pltpu.make_async_remote_copy(tok_own.at[pl.ds(a, n)], tok_peer.at[pl.ds(a, n)], ytok_ss.at[i],
                                         ytok_rs.at[i], device_id=peer, device_id_type=MESH)
            for i, (a, n) in enumerate(((0, cut), (cut, n_tok - cut)))]

    @pl.when(core == 0)
    def _():
        for cp in ytok:
            cp.start()

    for n in range(W_SLOTS):
        w_start(n)

    lane = 128
    tri = (lax.broadcasted_iota(jnp.int32, (lane, lane), 0)
           < lax.broadcasted_iota(jnp.int32, (lane, lane), 1)).astype(bf16)
    eye = (lax.broadcasted_iota(jnp.int32, (lane, lane), 0)
           == lax.broadcasted_iota(jnp.int32, (lane, lane), 1))
    exp_iota = lax.broadcasted_iota(jnp.int32, (n_exp, lane), 0)

    def route(ids, slots, column):
        counts = jnp.zeros((n_exp, 1), f32)
        for b in range(n_tok // lane):
            here = pl.ds(b * lane, lane)
            id_row = ids[:, here]
            hit = jnp.where(exp_iota == id_row, 1.0, 0.0).astype(f32)
            before = jnp.dot(hit.astype(bf16), tri, preferred_element_type=f32) + counts
            rank = jnp.sum(hit * before, axis=0, keepdims=True)
            counts = counts + jnp.sum(hit, axis=1, keepdims=True)
            slot = jnp.where(rank < cap, id_row.astype(f32) * cap + rank, -1.0)
            slots[:, here] = slot
            if column is not None:
                column[here, :] = jnp.sum(jnp.where(eye, slot, 0.0), axis=1, keepdims=True)

    route(ids_ref, slot_own, slot_col)
    ids_cp.wait_recv()
    route(ids_peer, slot_peer, None)

    @pl.when(core == 0)
    def _():
        ytok[0].wait_send()
        pl.semaphore_signal(go_sem, inc=1, device_id=partner, device_id_type=MESH)

    @pl.when(core == 1)
    def _():
        pl.semaphore_wait(go_sem, 1)
        for cp in ytok:
            cp.start()

    def disp_copy(e, d):
        return pltpu.make_async_remote_copy(
            send_rows.at[e, d - 1], rows.at[d % 2, e, pl.ds(2 * cap * (d // 2), 2 * cap)],
            disp_ss.at[e, d], disp_rs.at[e, d], device_id=dev(d), device_id_type=MESH)

    def dispatch():
        for cp in ytok:
            cp.wait_recv()

        def step(e, carry):
            k_iota = lax.broadcasted_iota(jnp.int32, (cap, 1), 0)
            target = jnp.concatenate([(k_iota + (rel_ep(d) * n_loc + e) * cap).astype(f32) for d in range(4)], axis=0)
            picked = []
            for slots, toks in ((slot_own, tok_own), (slot_peer, tok_peer)):
                pick = jnp.where(slots[...] == target, 1.0, 0.0).astype(bf16)
                picked.append(jnp.dot(pick, toks[...], preferred_element_type=f32))
            for d in range(4):
                part = slice(d * cap, (d + 1) * cap)
                block = jnp.concatenate([picked[0][part], picked[1][part]], axis=0).astype(bf16)
                if d == 0:
                    rows[0, e, pl.ds(0, 2 * cap)] = block
                else:
                    send_rows[e, d - 1] = block
            for d in (2, 3, 1):
                disp_copy(e, d).start()
            return carry

        lax.fori_loop(0, n_loc, step, 0)

    def part_copy(p, e, n):
        return pltpu.make_async_remote_copy(other.at[p, e], arrived.at[p, e], part_ss.at[n], part_rs.at[n],
                                            device_id=peer, device_id_type=MESH)

    def group_parity(g):
        return lax.rem(g + core, 2)

    def rows_wait(p, e, k):
        d = p + 2 * k
        pltpu.make_async_remote_copy(
            send_rows.at[0, 0], rows.at[p, e, pl.ds(2 * cap * k, 2 * cap)],
            disp_ss.at[e, d], disp_rs.at[e, d], device_id=peer, device_id_type=MESH).wait_recv()

    def experts(g):
        p = group_parity(g)

        def step(e, carry):
            n = g * n_loc + e
            slot = lax.rem(n, W_SLOTS)

            @pl.when(p == 1)
            def _():
                rows_wait(p, e, 0)
            rows_wait(p, e, 1)
            ups, downs = w_copies(n)
            ups.wait()
            x = rows[p, e]
            chunk = 512
            for j in range(ffn // chunk):
                cols = pl.ds(j * chunk, chunk)
                pre = jnp.dot(x, up_buf[slot, :, cols], preferred_element_type=f32)
                hid[:, cols] = jax.nn.gelu(pre, approximate=True).astype(bf16)
            downs.wait()
            part = jnp.dot(hid[...], down_buf[slot], preferred_element_type=f32)
            mine[p, e, pl.ds(0, cap)] = part[0:cap]
            other[p, e, pl.ds(0, cap)] = part[cap:2 * cap]
            mine[p, e, pl.ds(cap, cap)] = part[2 * cap:3 * cap]
            other[p, e, pl.ds(cap, cap)] = part[3 * cap:4 * cap]
            part_copy(p, e, n).start()

            @pl.when(n + W_SLOTS < 2 * n_loc)
            def _():
                w_start(n + W_SLOTS)
            return carry

        lax.fori_loop(0, n_loc, step, 0)

    @pl.when(core == 0)
    def _():
        dispatch()
    experts(0)

    @pl.when(core == 1)
    def _():
        dispatch()
    experts(1)

    def ret_copy(e, d):
        here = pl.ds(pl.multiple_of(d * pad, 16), pad)
        return pltpu.make_async_remote_copy(ret_send.at[e, d], ret_recv.at[e, here], ret_ss.at[e, d], ret_rs.at[e, d],
                                            device_id=dev(d), device_id_type=MESH)

    def reduce_step(g, e):
        p = group_parity(g)
        part_copy(p, e, g * n_loc + e).wait_recv()
        zeros = jnp.zeros((pad - cap, hidden), f32)
        blocks = []
        for k in range(2):
            here = pl.ds(k * cap, cap)
            total = mine[p, e, here] + arrived[p, e, here]
            blocks.append(jnp.concatenate([total, zeros], axis=0).astype(bf16))
        ret_send[e, p + 2] = blocks[1]
        ret_copy(e, p + 2).start()

        @pl.when(p == 0)
        def _():
            ret_recv[e, pl.ds(0, pad)] = blocks[0]

        @pl.when(p == 1)
        def _():
            ret_send[e, 1] = blocks[0]
            ret_copy(e, 1).start()

    out_rows = 256

    def combine(e, first):
        for d in (1, 2, 3):
            ret_copy(e, d).wait_recv()
        k_iota = lax.broadcasted_iota(jnp.int32, (1, 4 * pad), 1)
        block, rank = k_iota // pad, lax.rem(k_iota, pad)
        base = jnp.zeros((1, 4 * pad), jnp.int32)
        for d in range(4):
            base = base + jnp.where(block == d, (rel_ep(d) * n_loc + e) * cap, 0)
        target = jnp.where(rank < cap, base + rank, -2).astype(f32)

        def part(i, carry):
            here = pl.ds(pl.multiple_of(i * out_rows, out_rows), out_rows)
            pick = jnp.where(slot_col[here, :] == target, 1.0, 0.0).astype(bf16)
            got = jnp.dot(pick, ret_recv[e], preferred_element_type=f32)
            if first:
                out_ref[here, :] = got.astype(bf16)
            else:
                out_ref[here, :] = (out_ref[here, :].astype(f32) + got).astype(bf16)
            return carry

        lax.fori_loop(0, n_tok // out_rows, part, 0)

    def reduce_a(e, carry):
        reduce_step(0, e)
        return carry

    lax.fori_loop(0, n_loc, reduce_a, 0)

    @pl.when(core == 0)
    def _():
        combine(0, True)

        def rest(e, carry):
            combine(e, False)
            return carry

        lax.fori_loop(1, n_loc, rest, 0)

    reduce_step(1, 0)
    reduce_step(1, 1)

    @pl.when(core == 1)
    def _():
        combine(0, True)

    def reduce_b(e, carry):
        reduce_step(1, e)

        @pl.when(core == 1)
        def _():
            combine(e - 1, False)
        return carry

    lax.fori_loop(2, n_loc, reduce_b, 0)

    @pl.when(core == 1)
    def _():
        combine(n_loc - 1, False)

    ids_cp.wait_send()

    @pl.when(core == 1)
    def _():
        ytok[0].wait_send()
    ytok[1].wait_send()

    def drain(e, carry):
        for d in (1, 2, 3):
            disp_copy(e, d).wait_send()
            ret_copy(e, d).wait_send()
        for g in range(2):
            part_copy(g, e, g * n_loc + e).wait_send()
        return carry

    lax.fori_loop(0, n_loc, drain, 0)


def solution(mesh):
    n_ep, n_tp = mesh.shape['ep'], mesh.shape['tp']
    assert n_ep == 4 and n_tp == 2
    row_spec = P(('dp', 'ep', 'tp'), None)

    def local_moe(tokens, expert_ids, gate_vals, w_up, w_down):
        n_tok, hidden = tokens.shape
        n_loc, _, ffn = w_up.shape
        cap = capacity(n_tok, 1, n_loc * n_ep)
        pad = (cap + 15) // 16 * 16
        dims = (n_tok, hidden, ffn, n_loc, cap, pad)
        f32, bf16 = jnp.float32, jnp.bfloat16
        dma = pltpu.SemaphoreType.DMA
        vmem = pl.BlockSpec(memory_space=pltpu.VMEM)
        hbm = pl.BlockSpec(memory_space=pl.ANY)
        picked = pl.pallas_call(
            functools.partial(moe_kernel, dims),
            out_shape=jax.ShapeDtypeStruct((n_tok, hidden), bf16),
            in_specs=[hbm, vmem, hbm, hbm],
            out_specs=vmem,
            scratch_shapes=[
                pltpu.VMEM((n_tok, hidden), bf16),
                pltpu.VMEM((n_tok, hidden), bf16),
                pltpu.VMEM((1, n_tok), jnp.int32),
                pltpu.VMEM((1, n_tok), f32),
                pltpu.VMEM((1, n_tok), f32),
                pltpu.VMEM((n_tok, 1), f32),
                pltpu.VMEM((n_loc, 3, 2 * cap, hidden), bf16),
                pltpu.VMEM((2, n_loc, 4 * cap, hidden), bf16),
                pltpu.VMEM((W_SLOTS, hidden, ffn), bf16),
                pltpu.VMEM((W_SLOTS, ffn, hidden), bf16),
                pltpu.VMEM((4 * cap, ffn), bf16),
                pltpu.VMEM((2, n_loc, 2 * cap, hidden), f32),
                pltpu.VMEM((2, n_loc, 2 * cap, hidden), f32),
                pltpu.VMEM((2, n_loc, 2 * cap, hidden), f32),
                pltpu.VMEM((n_loc, 4, pad, hidden), bf16),
                pltpu.VMEM((n_loc, 4 * pad, hidden), bf16),
                dma, dma((W_SLOTS, 2)), dma, dma, dma((2,)), dma((2,)),
                dma((n_loc, 4)), dma((n_loc, 4)),
                dma((2 * n_loc,)), dma((2 * n_loc,)),
                dma((n_loc, 4)), dma((n_loc, 4)),
                pltpu.SemaphoreType.REGULAR,
            ],
            compiler_params=pltpu.CompilerParams(collective_id=0, has_side_effects=True, vmem_limit_bytes=62 << 20),
            name='moe_kernel',
        )(tokens, expert_ids.reshape(1, n_tok), w_up, w_down)
        return (gate_vals * picked.astype(f32)).astype(bf16)

    return jax.shard_map(local_moe, mesh=mesh,
                         in_specs=(row_spec, row_spec, row_spec, P('ep', None, 'tp'), P('ep', 'tp', None)),
                         out_specs=row_spec, check_vma=False)
```

```python
import functools

import jax
import jax.numpy as jnp
from jax import lax
from jax.experimental import pallas as pl
from jax.experimental.pallas import tpu as pltpu
from jax.sharding import PartitionSpec as P

MESH = pl.DeviceIdType.MESH
W_SLOTS = 2
VMEM_MIB = 52


def capacity(tok_count, n_top, n_exp):
    return ((5 * tok_count * n_top) // (4 * n_exp) + 7) // 8 * 8


def moe_kernel(dims, tok_hbm, ids_ref, up_hbm, down_hbm, out_ref,
               tok_own, tok_peer, ids_peer, slot_own, slot_peer, idx_col, cnts,
               send_rows, rows, up_buf, down_buf, hid, part, terms,
               ysend, arrived, mine, ovf, ret_recv,
               tok_sem, w_sem, ids_ss, ids_rs, ytok_ss, ytok_rs, cnt_ss, cnt_rs, disp_ss, disp_rs,
               d2d_ss, d2d_rs, ovf_ss, ovf_rs, y_ss, y_rs, ret_ss, ret_rs, go_sem, part_free):
    n_tok, hidden, ffn, n_loc, cap, pad = dims
    n_exp = 4 * n_loc
    col_exp = 2 * n_loc
    col_slots = col_exp * cap
    region = n_tok // 2
    quarter = region // 2
    chunk = quarter // 2
    n_ovf = col_slots - region
    f32, bf16, i32 = jnp.float32, jnp.bfloat16, jnp.int32
    dp, tp, ep = lax.axis_index('dp'), lax.axis_index('tp'), lax.axis_index('ep')
    core = lax.rem(ep, 2)
    col = ep // 2
    iota = functools.partial(lax.broadcasted_iota, i32)

    def rel_ep(d):
        flipped = lax.rem(ep + 2 * (d // 2), 4)
        return flipped + (d % 2) * (1 - 2 * lax.rem(flipped, 2))

    def dev(d, h=0):
        return (dp, tp if h == 0 else 1 - tp, rel_ep(d))

    peer = dev(0, 1)
    partner = dev(1)
    others = [(h, d) for d in range(4) for h in range(2) if (h, d) != (0, 0)]

    def remote(src, dst, ss, rs, target):
        return pltpu.make_async_remote_copy(src, dst, ss, rs, device_id=target, device_id_type=MESH)

    def parity(g):
        return lax.rem(g + core, 2)

    def w_copies(n):
        slot, e = lax.rem(n, W_SLOTS), lax.rem(n, n_loc)
        return (pltpu.make_async_copy(up_hbm.at[e], up_buf.at[slot], w_sem.at[slot, 0]),
                pltpu.make_async_copy(down_hbm.at[e], down_buf.at[slot], w_sem.at[slot, 1]))

    def w_start(n):
        for cp in w_copies(n):
            cp.start()

    tok_cp = pltpu.make_async_copy(tok_hbm, tok_own, tok_sem)
    tok_cp.start()

    barrier = pltpu.get_barrier_semaphore()
    for h, d in others:
        pl.semaphore_signal(barrier, inc=1, device_id=dev(d, h), device_id_type=MESH)
    pl.semaphore_wait(barrier, len(others))

    ids_cp = remote(ids_ref, ids_peer, ids_ss, ids_rs, peer)
    ids_cp.start()
    tok_cp.wait()

    cut = n_tok * 31 // 32
    ytok = [remote(tok_own.at[pl.ds(a, n)], tok_peer.at[pl.ds(a, n)], ytok_ss.at[i], ytok_rs.at[i], peer)
            for i, (a, n) in enumerate(((0, cut), (cut, n_tok - cut)))]

    @pl.when(core == 0)
    def _():
        for cp in ytok:
            cp.start()

    for n in range(W_SLOTS):
        w_start(n)

    lane = 128
    tri = (iota((lane, lane), 0) < iota((lane, lane), 1)).astype(bf16)
    eye = iota((lane, lane), 0) == iota((lane, lane), 1)
    exp_iota = iota((n_exp, lane), 0)
    row_e, col_e = iota((n_exp, n_exp), 0), iota((n_exp, n_exp), 1)
    before_in_col = ((col_e < row_e) & (col_e // col_exp == row_e // col_exp)).astype(bf16)

    def hits(ids, b):
        id_row = ids[:, pl.ds(b * lane, lane)]
        return id_row, jnp.where(exp_iota == id_row, 1.0, 0.0).astype(f32)

    def route(ids, slots):
        counts = jnp.zeros((n_exp, 1), f32)
        for b in range(n_tok // lane):
            id_row, hit = hits(ids, b)
            before = jnp.dot(hit.astype(bf16), tri, preferred_element_type=f32) + counts
            rank = jnp.sum(hit * before, axis=0, keepdims=True)
            counts = counts + jnp.sum(hit, axis=1, keepdims=True)
            slots[:, pl.ds(b * lane, lane)] = jnp.where(rank < cap, id_row.astype(f32) * cap + rank, -1.0)
        return counts

    def cnt_copy(h, d):
        return remote(cnts.at[0, 0], cnts.at[h, d], cnt_ss.at[h, d], cnt_rs.at[h, d], dev(d, h))

    kept = jnp.minimum(route(ids_ref, slot_own), float(cap))
    kept = jnp.broadcast_to(kept, (n_exp, lane))
    cnts[0, 0] = kept

    def disp_copy(h, e, d):
        return remote(send_rows.at[h, e, d - 1, pl.ds(0, cap)], rows.at[d % 2, e, 2 * h + d // 2, pl.ds(0, cap)],
                      disp_ss.at[h, e, d], disp_rs.at[h, e, d], dev(d))

    def disp_start(h, e):
        for d in (2, 3, 1):
            disp_copy(h, e, d).start()

    def dispatch(h):
        slots, toks = (slot_own, tok_own) if h == 0 else (slot_peer, tok_peer)

        def step(e2, carry):
            k_iota = iota((cap, 1), 0)
            pair = [(2 * e2 + m, d) for m in range(2) for d in range(4)]
            target = jnp.concatenate([(k_iota + (rel_ep(d) * n_loc + e) * cap).astype(f32) for e, d in pair], axis=0)
            pick = jnp.where(slots[...] == target, 1.0, 0.0).astype(bf16)
            picked = jnp.dot(pick, toks[...], preferred_element_type=f32)
            for m, (e, d) in enumerate(pair):
                block = picked[m * cap:(m + 1) * cap].astype(bf16)
                if d == 0:
                    rows[0, e, 2 * h, pl.ds(0, cap)] = block
                else:
                    send_rows[h, e, d - 1, pl.ds(0, cap)] = block
            for m in range(2):
                if h == 1:
                    disp_start(h, 2 * e2 + m)
                else:
                    @pl.when((core == 0) | (e2 < n_loc // 4))
                    def _():
                        disp_start(h, 2 * e2 + m)
            return carry

        lax.fori_loop(0, n_loc // 2, step, 0)

    dispatch(0)

    for h, d in others:
        cnt_copy(h, d).start()

    first_row = jnp.dot(before_in_col, kept.astype(bf16), preferred_element_type=f32)
    for b in range(n_tok // lane):
        here = pl.ds(b * lane, lane)
        id_row, hit = hits(ids_ref, b)
        slot = slot_own[:, here]
        rank = slot - id_row.astype(f32) * cap
        joint = (jnp.sum(hit * first_row, axis=0, keepdims=True) + rank).astype(i32)
        home = id_row // col_exp
        stays = joint < region
        where_col = jnp.where(stays, home, 1 - home)
        q = jnp.where(stays, joint, 2 * region - 1 - joint)
        idx = lax.rem(q // chunk, 2) * region + (2 * where_col + q // quarter) * chunk + lax.rem(q, chunk)
        idx = jnp.where(slot < 0.0, -1.0, idx.astype(f32))
        idx_col[here, :] = jnp.sum(jnp.where(eye, idx, 0.0), axis=1, keepdims=True)

    ids_cp.wait_recv()
    route(ids_peer, slot_peer)

    @pl.when(core == 0)
    def _():
        ytok[0].wait_send()
        pl.semaphore_signal(go_sem, inc=1, device_id=partner, device_id_type=MESH)

    @pl.when(core == 1)
    def _():
        pl.semaphore_wait(go_sem, 1)
        for cp in ytok:
            cp.start()

    def d2d_copy(h, g, e):
        here = pl.ds(pl.multiple_of((core * n_loc + e) * cap, 8), cap)
        half = pl.ds(2 * h, 2)
        return remote(part.at[half, here], part.at[half, here], d2d_ss.at[h, g, e], d2d_rs.at[h, g, e], partner)

    def experts(g, extra):
        p = parity(g)

        def arrival(h, e, k):
            d = p + 2 * k
            remote(send_rows.at[0, 0, 0, pl.ds(0, cap)], rows.at[p, e, 2 * h + k, pl.ds(0, cap)],
                   disp_ss.at[h, e, d], disp_rs.at[h, e, d], peer).wait_recv()

        def step(e, carry):
            n = g * n_loc + e
            slot = lax.rem(n, W_SLOTS)
            for h in range(2):
                @pl.when(p == 1)
                def _():
                    arrival(h, e, 0)
                arrival(h, e, 1)
            ups, downs = w_copies(n)
            ups.wait()
            x = rows[p, e].reshape(4 * pad, hidden)
            width = 512
            for j in range(ffn // width):
                cols = pl.ds(j * width, width)
                pre = jnp.dot(x, up_buf[slot, :, cols], preferred_element_type=f32)
                hid[:, cols] = jax.nn.gelu(pre, approximate=True).astype(bf16)
            downs.wait()
            res = jnp.dot(hid[...], down_buf[slot], preferred_element_type=f32)
            here = pl.ds(pl.multiple_of((core * n_loc + e) * cap, 8), cap)
            for hk in range(4):
                part[hk, here] = res[hk * pad:hk * pad + cap]
            d2d_copy(1, g, e).start()
            d2d_copy(0, g, e).start()

            @pl.when(n + W_SLOTS < 2 * n_loc)
            def _():
                w_start(n + W_SLOTS)
            extra(e)
            return carry

        lax.fori_loop(0, n_loc, step, 0)

    slot_iota = iota((1, col_slots), 1)
    slot_exp, slot_rank = slot_iota // cap, lax.rem(slot_iota, cap)
    exp_match = iota((col_exp, col_slots), 0) == slot_exp
    before_exp = (iota((col_exp, col_exp), 1) < iota((col_exp, col_exp), 0)).astype(bf16)

    def positions(h, p, k):
        cnt = cnts[h, p + 2 * k, pl.ds(pl.multiple_of(col * col_exp, 8), col_exp), :]
        start = jnp.dot(before_exp, cnt.astype(bf16), preferred_element_type=f32)
        start_row = jnp.sum(jnp.where(exp_match, start[:, 0:1], 0.0), axis=0, keepdims=True)
        cnt_row = jnp.sum(jnp.where(exp_match, cnt[:, 0:1], 0.0), axis=0, keepdims=True)
        rank = slot_rank.astype(f32)
        return jnp.where(rank < cnt_row, start_row + rank, -1.0)

    def ovf_copy(h, g, k):
        p = parity(g)
        return remote(ovf.at[h, p, k], ovf.at[h, 1 - p, 1 - k], ovf_ss.at[h, g, k], ovf_rs.at[h, g, 1 - k], dev(3))

    def y_copy(p, k, i):
        here = pl.ds(i * chunk, chunk)
        return remote(ysend.at[p, k, here], arrived.at[p, k, here], y_ss.at[p, k, i], y_rs.at[p, k, i], peer)

    def compact(h, g):
        p = parity(g)
        dest = ysend if h == 1 else mine

        for k in (1, 0):
            where = positions(h, p, k)
            x = part[2 * h + k]
            hi = x.astype(bf16)
            rest = x - hi.astype(f32)
            mid = rest.astype(bf16)
            terms[pl.ds(0, col_slots)] = hi
            terms[pl.ds(col_slots, col_slots)] = mid
            terms[pl.ds(2 * col_slots, col_slots)] = (rest - mid.astype(f32)).astype(bf16)

            def take(target):
                pick = jnp.where(where == target.astype(f32), 1.0, 0.0).astype(bf16)
                return jnp.dot(jnp.concatenate([pick] * 3, axis=1), terms[...], preferred_element_type=f32)

            row = iota((quarter, 1), 0) + core * quarter

            @pl.when(core == 0)
            def _():
                got = take(jnp.concatenate([row, (col_slots - 1) - iota((n_ovf, 1), 0)], axis=0))
                dest[p, k] = got[0:quarter]
                ovf[h, p, k] = got[quarter:quarter + n_ovf]
                if h == 1:
                    y_copy(p, k, 0).start()
                    y_copy(p, k, 1).start()
                    ovf_copy(h, g, k).start()

            @pl.when(core == 1)
            def _():
                dest[p, k] = take(row)
                if h == 1:
                    y_copy(p, k, 0).start()

    def ovf_start(h, g):
        for k in (1, 0):
            ovf_copy(h, g, k).start()

    def d2d_wait(h, g):
        def wait(e, carry):
            d2d_copy(h, g, e).wait_recv()
            return carry

        lax.fori_loop(0, n_loc, wait, 0)

    def fill(h, g):
        p = parity(g)
        dest = ysend if h == 1 else mine

        @pl.when(core == 1)
        def _():
            for k in (1, 0):
                here = pl.ds(quarter - n_ovf, n_ovf)
                ovf_copy(h, g, 1 - k).wait_recv()
                dest[p, k, here] = dest[p, k, here] + ovf[h, p, k]
                if h == 1:
                    y_copy(p, k, 1).start()

    def ret_rows(p, k, i):
        start = (2 * p + k) * quarter + i * chunk
        return tok_peer.at[pl.ds(pl.multiple_of(start, chunk), chunk)]

    def ret_copy(p, k, i):
        d = p + 2 * k
        there = pl.ds(pl.multiple_of(i * region + ep * chunk, chunk), chunk)
        return remote(ret_rows(p, k, i), ret_recv.at[there], ret_ss.at[p, k, i], ret_rs.at[d, i], dev(d))

    def ret_wait(d, i):
        remote(tok_peer.at[pl.ds(0, chunk)], ret_recv.at[pl.ds(0, chunk)], ret_ss.at[0, 0, 0], ret_rs.at[d, i],
               peer).wait_recv()

    def reduce_chunk(g, k, i):
        p = parity(g)
        here = pl.ds(i * chunk, chunk)
        y_copy(p, k, i).wait_recv()
        total = (mine[p, k, here] + arrived[p, k, here]).astype(bf16)
        if k == 1:
            ret_rows(p, k, i)[...] = total
            ret_copy(p, k, i).start()
        else:
            @pl.when(p == 0)
            def _():
                ret_recv[pl.ds(pl.multiple_of(i * region + ep * chunk, chunk), chunk)] = total

            @pl.when(p == 1)
            def _():
                ret_rows(p, k, i)[...] = total
                ret_copy(p, k, i).start()

    out_rows = 256

    def combine(far, i, first=False):
        for d in ((2, 3) if far else (1,)):
            ret_wait(d, i)
        start = i * region + (lax.rem(col + far, 2)) * 2 * chunk
        here_r = pl.ds(pl.multiple_of(start, chunk), 2 * chunk)
        target = (iota((1, 2 * chunk), 1) + start).astype(f32)

        def some(j, carry):
            here = pl.ds(pl.multiple_of(j * out_rows, out_rows), out_rows)
            pick = jnp.where(idx_col[here, :] == target, 1.0, 0.0).astype(bf16)
            got = jnp.dot(pick, ret_recv[here_r, :], preferred_element_type=f32)
            if first:
                out_ref[here, :] = got.astype(bf16)
            else:
                out_ref[here, :] = (out_ref[here, :].astype(f32) + got).astype(bf16)
            return carry

        lax.fori_loop(0, n_tok // out_rows, some, 0)

    @pl.when(core == 0)
    def _():
        for cp in ytok:
            cp.wait_recv()
        dispatch(1)

    def during_b(e):
        @pl.when(e == n_loc // 2)
        def _():
            fill(1, 0)

            @pl.when(core == 0)
            def _():
                ovf_start(0, 0)

    experts(0, lambda e: None)

    @pl.when(core == 1)
    def _():
        for e in range(n_loc // 2, n_loc):
            disp_start(0, e)
    d2d_wait(1, 0)
    for h, d in others:
        cnt_copy(h, d).wait_recv()
    compact(1, 0)

    @pl.when(core == 1)
    def _():
        for cp in ytok:
            cp.wait_recv()
        dispatch(1)
    d2d_wait(0, 0)
    compact(0, 0)
    pl.semaphore_signal(part_free, inc=1, device_id=partner, device_id_type=MESH)
    pl.semaphore_wait(part_free, 1)

    def sent_a(e, carry):
        for h in range(2):
            d2d_copy(h, 0, e).wait_send()
        return carry

    lax.fori_loop(0, n_loc, sent_a, 0)
    experts(1, during_b)
    d2d_wait(1, 1)
    compact(1, 1)
    fill(0, 0)

    @pl.when(core == 0)
    def _():
        for k, i in ((1, 0), (1, 1), (0, 0), (0, 1)):
            reduce_chunk(0, k, i)

    @pl.when(core == 1)
    def _():
        for k, i in ((1, 0), (0, 0), (1, 1), (0, 1)):
            reduce_chunk(0, k, i)
    d2d_wait(0, 1)
    compact(0, 1)

    @pl.when(core == 0)
    def _():
        ovf_start(0, 1)
        reduce_chunk(1, 1, 0)
        reduce_chunk(1, 1, 1)
        combine(1, 0, True)
        combine(0, 0)
        combine(1, 1)
        combine(0, 1)
        reduce_chunk(1, 0, 0)
        reduce_chunk(1, 0, 1)

    @pl.when(core == 1)
    def _():
        fill(1, 1)
        reduce_chunk(1, 1, 0)
        reduce_chunk(1, 0, 0)
        fill(0, 1)
        combine(1, 0, True)
        reduce_chunk(1, 1, 1)
        combine(0, 0)
        combine(1, 1)
        reduce_chunk(1, 0, 1)
        combine(0, 1)

    ids_cp.wait_send()

    @pl.when(core == 1)
    def _():
        ytok[0].wait_send()
    ytok[1].wait_send()
    for h, d in others:
        cnt_copy(h, d).wait_send()

    def drain(e, carry):
        for h in range(2):
            for d in (1, 2, 3):
                disp_copy(h, e, d).wait_send()
            d2d_copy(h, 1, e).wait_send()
        return carry

    lax.fori_loop(0, n_loc, drain, 0)

    @pl.when(core == 0)
    def _():
        for h in range(2):
            for g in range(2):
                for k in range(2):
                    ovf_copy(h, g, k).wait_send()
    for i in range(2):
        for p in range(2):
            for k in range(2):
                y_copy(p, k, i).wait_send()
                if p + 2 * k > 0:
                    ret_copy(p, k, i).wait_send()


def solution(mesh):
    n_ep, n_tp = mesh.shape['ep'], mesh.shape['tp']
    assert n_ep == 4 and n_tp == 2
    row_spec = P(('dp', 'ep', 'tp'), None)

    def local_moe(tokens, expert_ids, gate_vals, w_up, w_down):
        n_tok, hidden = tokens.shape
        n_loc, _, ffn = w_up.shape
        cap = capacity(n_tok, 1, n_loc * n_ep)
        pad = (cap + 15) // 16 * 16
        dims = (n_tok, hidden, ffn, n_loc, cap, pad)
        quarter = n_tok // 4
        col_slots = 2 * n_loc * cap
        n_ovf = col_slots - 2 * quarter
        f32, bf16 = jnp.float32, jnp.bfloat16
        dma = pltpu.SemaphoreType.DMA
        vmem = pl.BlockSpec(memory_space=pltpu.VMEM)
        hbm = pl.BlockSpec(memory_space=pl.ANY)
        picked = pl.pallas_call(
            functools.partial(moe_kernel, dims),
            out_shape=jax.ShapeDtypeStruct((n_tok, hidden), bf16),
            in_specs=[hbm, vmem, hbm, hbm],
            out_specs=vmem,
            scratch_shapes=[
                pltpu.VMEM((n_tok, hidden), bf16),
                pltpu.VMEM((n_tok, hidden), bf16),
                pltpu.VMEM((1, n_tok), jnp.int32),
                pltpu.VMEM((1, n_tok), f32),
                pltpu.VMEM((1, n_tok), f32),
                pltpu.VMEM((n_tok, 1), f32),
                pltpu.VMEM((2, 4, 4 * n_loc, 128), f32),
                pltpu.VMEM((2, n_loc, 3, pad, hidden), bf16),
                pltpu.VMEM((2, n_loc, 4, pad, hidden), bf16),
                pltpu.VMEM((W_SLOTS, hidden, ffn), bf16),
                pltpu.VMEM((W_SLOTS, ffn, hidden), bf16),
                pltpu.VMEM((4 * pad, ffn), bf16),
                pltpu.VMEM((4, col_slots, hidden), f32),
                pltpu.VMEM((3 * col_slots, hidden), bf16),
                pltpu.VMEM((2, 2, quarter, hidden), f32),
                pltpu.VMEM((2, 2, quarter, hidden), f32),
                pltpu.VMEM((2, 2, quarter, hidden), f32),
                pltpu.VMEM((2, 2, 2, n_ovf, hidden), f32),
                pltpu.VMEM((n_tok, hidden), bf16),
                dma, dma((W_SLOTS, 2)), dma, dma, dma((2,)), dma((2,)), dma((2, 4)), dma((2, 4)),
                dma((2, n_loc, 4)), dma((2, n_loc, 4)),
                dma((2, 2, n_loc)), dma((2, 2, n_loc)),
                dma((2, 2, 2)), dma((2, 2, 2)),
                dma((2, 2, 2)), dma((2, 2, 2)),
                dma((2, 2, 2)), dma((4, 2)),
                pltpu.SemaphoreType.REGULAR,
                pltpu.SemaphoreType.REGULAR,
            ],
            compiler_params=pltpu.CompilerParams(collective_id=0, has_side_effects=True, vmem_limit_bytes=VMEM_MIB << 20),
            name='moe_kernel',
        )(tokens, expert_ids.reshape(1, n_tok), w_up, w_down)
        return (gate_vals * picked.astype(f32)).astype(bf16)

    return jax.shard_map(local_moe, mesh=mesh,
                         in_specs=(row_spec, row_spec, row_spec, P('ep', None, 'tp'), P('ep', 'tp', None)),
                         out_specs=row_spec, check_vma=False)
```

```python
import functools

import jax
import jax.numpy as jnp
from jax import lax
from jax.experimental import pallas as pl
from jax.experimental.pallas import tpu as pltpu
from jax.sharding import PartitionSpec as P

MESH = pl.DeviceIdType.MESH
W_SLOTS = 2
VMEM_MIB = 52


def capacity(tok_count, n_top, n_exp):
    return ((5 * tok_count * n_top) // (4 * n_exp) + 7) // 8 * 8


def moe_kernel(dims, tok_hbm, ids_hbm, up_hbm, down_hbm, out_ref,
               tok_own, tok_peer, ids_ref, ids_peer, slot_own, slot_peer, idx_col, cnts,
               send_rows, rows, up_buf, down_buf, hid, part, terms,
               ysend, arrived, mine, ovf, ret_recv,
               tok_sem, ids_sem, w_sem, ids_ss, ids_rs, ytok_ss, ytok_rs, cnt_ss, cnt_rs, disp_ss, disp_rs,
               d2d_ss, d2d_rs, ovf_ss, ovf_rs, y_ss, y_rs, ret_ss, ret_rs, go_sem, part_free):
    n_tok, hidden, ffn, n_loc, cap, pad = dims
    n_exp = 4 * n_loc
    col_exp = 2 * n_loc
    col_slots = col_exp * cap
    region = n_tok // 2
    quarter = region // 2
    chunk = quarter // 2
    n_ovf = col_slots - region
    f32, bf16, i32 = jnp.float32, jnp.bfloat16, jnp.int32
    dp, tp, ep = lax.axis_index('dp'), lax.axis_index('tp'), lax.axis_index('ep')
    core = lax.rem(ep, 2)
    col = ep // 2
    iota = functools.partial(lax.broadcasted_iota, i32)

    def rel_ep(d):
        flipped = lax.rem(ep + 2 * (d // 2), 4)
        return flipped + (d % 2) * (1 - 2 * lax.rem(flipped, 2))

    def dev(d, h=0):
        return (dp, tp if h == 0 else 1 - tp, rel_ep(d))

    peer = dev(0, 1)
    partner = dev(1)
    others = [(h, d) for d in range(4) for h in range(2) if (h, d) != (0, 0)]

    def remote(src, dst, ss, rs, target):
        return pltpu.make_async_remote_copy(src, dst, ss, rs, device_id=target, device_id_type=MESH)

    def parity(g):
        return lax.rem(g + core, 2)

    def w_copies(n):
        slot, e = lax.rem(n, W_SLOTS), lax.rem(n, n_loc)
        halves = []
        for i, (src, dst) in enumerate(((up_hbm, up_buf), (down_hbm, down_buf))):
            size = src.shape[1] // 2
            halves.append([pltpu.make_async_copy(src.at[e, pl.ds(m * size, size)], dst.at[slot, pl.ds(m * size, size)],
                                                 w_sem.at[slot, i, m]) for m in range(2)])
        return halves

    def for_all(what, copies):
        for cp in copies:
            getattr(cp, what)()

    def w_start(n):
        for half in w_copies(n):
            for cp in half:
                cp.start()

    tok_cp = pltpu.make_async_copy(tok_hbm, tok_own, tok_sem)
    tok_cp.start()
    ids_load = pltpu.make_async_copy(ids_hbm, ids_ref, ids_sem)
    ids_load.start()

    barrier = pltpu.get_barrier_semaphore()
    for h, d in others:
        pl.semaphore_signal(barrier, inc=1, device_id=dev(d, h), device_id_type=MESH)
    pl.semaphore_wait(barrier, len(others))

    ids_load.wait()
    ids_cp = remote(ids_ref, ids_peer, ids_ss, ids_rs, peer)
    ids_cp.start()
    tok_cp.wait()

    cut = n_tok * 31 // 32
    ytok = [remote(tok_own.at[pl.ds(a, n)], tok_peer.at[pl.ds(a, n)], ytok_ss.at[i], ytok_rs.at[i], peer)
            for i, (a, n) in enumerate(((0, cut), (cut, n_tok - cut)))]

    @pl.when(core == 0)
    def _():
        for cp in ytok:
            cp.start()

    for n in range(W_SLOTS):
        w_start(n)

    lane = 128
    tri = (iota((lane, lane), 0) < iota((lane, lane), 1)).astype(bf16)
    eye = iota((lane, lane), 0) == iota((lane, lane), 1)
    exp_iota = iota((n_exp, lane), 0)
    row_e, col_e = iota((n_exp, n_exp), 0), iota((n_exp, n_exp), 1)
    before_in_col = ((col_e < row_e) & (col_e // col_exp == row_e // col_exp)).astype(bf16)

    def hits(ids, b):
        id_row = ids[:, pl.ds(b * lane, lane)]
        return id_row, jnp.where(exp_iota == id_row, 1.0, 0.0).astype(f32)

    def route(ids, slots):
        counts = jnp.zeros((n_exp, 1), f32)
        for b in range(n_tok // lane):
            id_row, hit = hits(ids, b)
            before = jnp.dot(hit.astype(bf16), tri, preferred_element_type=f32) + counts
            rank = jnp.sum(hit * before, axis=0, keepdims=True)
            counts = counts + jnp.sum(hit, axis=1, keepdims=True)
            slots[:, pl.ds(b * lane, lane)] = jnp.where(rank < cap, id_row.astype(f32) * cap + rank, -1.0)
        return counts

    def cnt_copy(h, d):
        return remote(cnts.at[0], cnts.at[4 * h + d], cnt_ss, cnt_rs, dev(d, h))

    kept = jnp.minimum(route(ids_ref, slot_own), float(cap))
    kept = jnp.broadcast_to(kept, (n_exp, lane))
    cnts[0] = kept

    def disp_copy(h, e, d):
        return remote(send_rows.at[h, e, d - 1, pl.ds(0, cap)], rows.at[d % 2, e, 2 * h + d // 2, pl.ds(0, cap)],
                      disp_ss.at[h], disp_rs.at[d % 2, e], dev(d))

    def disp_start(h, e):
        for d in (2, 3, 1):
            disp_copy(h, e, d).start()

    def dispatch(h):
        slots, toks = (slot_own, tok_own) if h == 0 else (slot_peer, tok_peer)

        def step(e2, carry):
            k_iota = iota((cap, 1), 0)
            pair = [(2 * e2 + m, d) for m in range(2) for d in range(4)]
            target = jnp.concatenate([(k_iota + (rel_ep(d) * n_loc + e) * cap).astype(f32) for e, d in pair], axis=0)
            pick = jnp.where(slots[...] == target, 1.0, 0.0).astype(bf16)
            picked = jnp.dot(pick, toks[...], preferred_element_type=f32)
            for m, (e, d) in enumerate(pair):
                block = picked[m * cap:(m + 1) * cap].astype(bf16)
                if d == 0:
                    rows[0, e, 2 * h, pl.ds(0, cap)] = block
                else:
                    send_rows[h, e, d - 1, pl.ds(0, cap)] = block
            for m in range(2):
                if h == 1:
                    disp_start(h, 2 * e2 + m)
                else:
                    @pl.when((core == 0) | (e2 < n_loc // 4))
                    def _():
                        disp_start(h, 2 * e2 + m)
            return carry

        lax.fori_loop(0, n_loc // 2, step, 0)

    dispatch(0)

    for h, d in others:
        cnt_copy(h, d).start()

    first_row = jnp.dot(before_in_col, kept.astype(bf16), preferred_element_type=f32)
    for b in range(n_tok // lane):
        here = pl.ds(b * lane, lane)
        id_row, hit = hits(ids_ref, b)
        slot = slot_own[:, here]
        rank = slot - id_row.astype(f32) * cap
        joint = (jnp.sum(hit * first_row, axis=0, keepdims=True) + rank).astype(i32)
        home = id_row // col_exp
        stays = joint < region
        where_col = jnp.where(stays, home, 1 - home)
        q = jnp.where(stays, joint, 2 * region - 1 - joint)
        idx = lax.rem(q // chunk, 2) * region + (2 * where_col + q // quarter) * chunk + lax.rem(q, chunk)
        idx = jnp.where(slot < 0.0, -1.0, idx.astype(f32))
        idx_col[here, :] = jnp.sum(jnp.where(eye, idx, 0.0), axis=1, keepdims=True)

    ids_cp.wait_recv()
    route(ids_peer, slot_peer)

    @pl.when(core == 0)
    def _():
        ytok[0].wait_send()
        pl.semaphore_signal(go_sem, inc=1, device_id=partner, device_id_type=MESH)

    @pl.when(core == 1)
    def _():
        pl.semaphore_wait(go_sem, 1)
        for cp in ytok:
            cp.start()

    def d2d_copy(h, g, e):
        here = pl.ds(pl.multiple_of((core * n_loc + e) * cap, 8), cap)
        half = pl.ds(2 * h, 2)
        return remote(part.at[half, here], part.at[half, here], d2d_ss.at[h, g], d2d_rs.at[h, g], partner)

    def experts(g, extra):
        p = parity(g)

        def arrival(e, blocks):
            here = rows.at[p, e, pl.ds(0, blocks), pl.ds(0, cap)]
            remote(here, here, disp_ss.at[0], disp_rs.at[p, e], peer).wait_recv()

        def step(e, carry):
            n = g * n_loc + e
            slot = lax.rem(n, W_SLOTS)

            @pl.when(p == 1)
            def _():
                arrival(e, 4)

            @pl.when(p == 0)
            def _():
                arrival(e, 2)
            ups, downs = w_copies(n)
            for_all('wait', ups)
            x = rows[p, e].reshape(4 * pad, hidden)
            width = 512
            for j in range(ffn // width):
                cols = pl.ds(j * width, width)
                pre = jnp.dot(x, up_buf[slot, :, cols], preferred_element_type=f32)
                hid[:, cols] = jax.nn.gelu(pre, approximate=True).astype(bf16)

            @pl.when(n + W_SLOTS < 2 * n_loc)
            def _():
                for_all('start', w_copies(n + W_SLOTS)[0])
            for_all('wait', downs)
            res = jnp.dot(hid[...], down_buf[slot], preferred_element_type=f32)
            here = pl.ds(pl.multiple_of((core * n_loc + e) * cap, 8), cap)
            for hk in range(4):
                part[hk, here] = res[hk * pad:hk * pad + cap]
            d2d_copy(1, g, e).start()
            d2d_copy(0, g, e).start()

            @pl.when(n + W_SLOTS < 2 * n_loc)
            def _():
                for_all('start', w_copies(n + W_SLOTS)[1])
            extra(e)
            return carry

        lax.fori_loop(0, n_loc, step, 0)

    slot_iota = iota((1, col_slots), 1)
    slot_exp, slot_rank = slot_iota // cap, lax.rem(slot_iota, cap)
    exp_match = iota((col_exp, col_slots), 0) == slot_exp
    before_exp = (iota((col_exp, col_exp), 1) < iota((col_exp, col_exp), 0)).astype(bf16)

    def positions(h, p, k):
        cnt = cnts[4 * h + p + 2 * k, pl.ds(pl.multiple_of(col * col_exp, 8), col_exp), :]
        start = jnp.dot(before_exp, cnt.astype(bf16), preferred_element_type=f32)
        start_row = jnp.sum(jnp.where(exp_match, start[:, 0:1], 0.0), axis=0, keepdims=True)
        cnt_row = jnp.sum(jnp.where(exp_match, cnt[:, 0:1], 0.0), axis=0, keepdims=True)
        rank = slot_rank.astype(f32)
        return jnp.where(rank < cnt_row, start_row + rank, -1.0)

    def ovf_copy(h, g, k):
        p = parity(g)
        return remote(ovf.at[h, p, k], ovf.at[h, 1 - p, 1 - k], ovf_ss.at[h], ovf_rs.at[h, g, 1 - k], dev(3))

    def y_copy(p, k, i):
        here = pl.ds(i * chunk, chunk)
        return remote(ysend.at[p, k, here], arrived.at[p, k, here], y_ss.at[p], y_rs.at[p, k, i], peer)

    def compact(h, g):
        p = parity(g)
        dest = ysend if h == 1 else mine

        for k in (1, 0):
            where = positions(h, p, k)
            x = part[2 * h + k]
            hi = x.astype(bf16)
            rest = x - hi.astype(f32)
            mid = rest.astype(bf16)
            terms[pl.ds(0, col_slots)] = hi
            terms[pl.ds(col_slots, col_slots)] = mid
            terms[pl.ds(2 * col_slots, col_slots)] = (rest - mid.astype(f32)).astype(bf16)

            def take(target):
                pick = jnp.where(where == target.astype(f32), 1.0, 0.0).astype(bf16)
                return jnp.dot(jnp.concatenate([pick] * 3, axis=1), terms[...], preferred_element_type=f32)

            row = iota((quarter, 1), 0) + core * quarter

            @pl.when(core == 0)
            def _():
                got = take(jnp.concatenate([row, (col_slots - 1) - iota((n_ovf, 1), 0)], axis=0))
                dest[p, k] = got[0:quarter]
                ovf[h, p, k] = got[quarter:quarter + n_ovf]
                if h == 1:
                    y_copy(p, k, 0).start()
                    y_copy(p, k, 1).start()
                    ovf_copy(h, g, k).start()

            @pl.when(core == 1)
            def _():
                dest[p, k] = take(row)
                if h == 1 and (g == 0 or k == 1):
                    y_copy(p, k, 0).start()

    def ovf_start(h, g):
        for k in (1, 0):
            ovf_copy(h, g, k).start()

    half_col = n_loc * cap

    def d2d_all(h, g):
        here = part.at[pl.ds(2 * h, 2), pl.ds(0, half_col)]
        return remote(here, here, d2d_ss.at[h, g], d2d_rs.at[h, g], partner)

    def d2d_wait(h, g):
        d2d_all(h, g).wait_recv()

    def d2d_drain(g):
        for h in range(2):
            d2d_all(h, g).wait_send()

    def fill(h, g):
        p = parity(g)
        dest = ysend if h == 1 else mine

        @pl.when(core == 1)
        def _():
            for k in (1, 0):
                here = pl.ds(quarter - n_ovf, n_ovf)
                ovf_copy(h, g, 1 - k).wait_recv()
                dest[p, k, here] = dest[p, k, here] + ovf[h, p, k]
                if h == 1:
                    if g == 1 and k == 0:
                        y_copy(p, k, 0).start()
                    y_copy(p, k, 1).start()

    def ret_rows(p, k, i):
        start = (2 * p + k) * quarter + i * chunk
        return tok_peer.at[pl.ds(pl.multiple_of(start, chunk), chunk)]

    def ret_copy(p, k, i):
        d = p + 2 * k
        there = pl.ds(pl.multiple_of(i * region + ep * chunk, chunk), chunk)
        return remote(ret_rows(p, k, i), ret_recv.at[there], ret_ss, ret_rs.at[d, i], dev(d))

    def ret_wait(d, i):
        remote(tok_peer.at[pl.ds(0, chunk)], ret_recv.at[pl.ds(0, chunk)], ret_ss, ret_rs.at[d, i],
               peer).wait_recv()

    def reduce_chunk(g, k, i):
        p = parity(g)
        here = pl.ds(i * chunk, chunk)
        y_copy(p, k, i).wait_recv()
        total = (mine[p, k, here] + arrived[p, k, here]).astype(bf16)
        if k == 1:
            ret_rows(p, k, i)[...] = total
            ret_copy(p, k, i).start()
        else:
            @pl.when(p == 0)
            def _():
                ret_recv[pl.ds(pl.multiple_of(i * region + ep * chunk, chunk), chunk)] = total

            @pl.when(p == 1)
            def _():
                ret_rows(p, k, i)[...] = total
                ret_copy(p, k, i).start()

    out_rows = 256

    def combine(far, i, first=False):
        for d in ((2, 3) if far else (1,)):
            ret_wait(d, i)
        start = i * region + (lax.rem(col + far, 2)) * 2 * chunk
        here_r = pl.ds(pl.multiple_of(start, chunk), 2 * chunk)
        target = (iota((1, 2 * chunk), 1) + start).astype(f32)

        for j in range(n_tok // out_rows):
            here = pl.ds(j * out_rows, out_rows)
            pick = jnp.where(idx_col[here, :] == target, 1.0, 0.0).astype(bf16)
            got = jnp.dot(pick, ret_recv[here_r, :], preferred_element_type=f32)
            if first:
                out_ref[here, :] = got.astype(bf16)
            else:
                out_ref[here, :] = (out_ref[here, :].astype(f32) + got).astype(bf16)

    @pl.when(core == 0)
    def _():
        for cp in ytok:
            cp.wait_recv()
        dispatch(1)

    def during_b(e):
        @pl.when(e == n_loc // 2)
        def _():
            fill(1, 0)

            @pl.when(core == 0)
            def _():
                ovf_start(0, 0)

    experts(0, lambda e: None)

    @pl.when(core == 1)
    def _():
        for e in range(n_loc // 2, n_loc):
            disp_start(0, e)
    d2d_wait(1, 0)
    cnt_all = remote(cnts.at[pl.ds(1, 7)], cnts.at[pl.ds(1, 7)], cnt_ss, cnt_rs, peer)
    cnt_all.wait_recv()
    compact(1, 0)

    @pl.when(core == 1)
    def _():
        for cp in ytok:
            cp.wait_recv()
        dispatch(1)
    d2d_wait(0, 0)
    compact(0, 0)
    pl.semaphore_signal(part_free, inc=1, device_id=partner, device_id_type=MESH)
    pl.semaphore_wait(part_free, 1)

    d2d_drain(0)
    experts(1, during_b)
    d2d_wait(1, 1)
    compact(1, 1)
    d2d_wait(0, 1)
    compact(0, 1)

    @pl.when(core == 0)
    def _():
        ovf_start(0, 1)
        for k, i in ((1, 0), (1, 1), (0, 0), (0, 1)):
            reduce_chunk(0, k, i)

    @pl.when(core == 1)
    def _():
        fill(0, 0)
        for k, i in ((1, 0), (0, 0), (1, 1)):
            reduce_chunk(0, k, i)
        fill(1, 1)
        reduce_chunk(0, 0, 1)

    ids_cp.wait_send()

    @pl.when(core == 1)
    def _():
        ytok[0].wait_send()
    ytok[1].wait_send()
    cnt_all.wait_send()

    for h in range(2):
        sent = send_rows.at[h, :, :, pl.ds(0, cap)]
        remote(sent, sent, disp_ss.at[h], disp_rs.at[0, 0], peer).wait_send()
    d2d_drain(1)

    @pl.when(core == 0)
    def _():
        reduce_chunk(1, 1, 0)
        reduce_chunk(1, 1, 1)
        combine(1, 0, True)
        combine(0, 0)
        combine(1, 1)
        combine(0, 1)
        reduce_chunk(1, 0, 0)
        reduce_chunk(1, 0, 1)

    @pl.when(core == 1)
    def _():
        reduce_chunk(1, 1, 0)
        fill(0, 1)
        combine(1, 0, True)
        reduce_chunk(1, 1, 1)
        reduce_chunk(1, 0, 0)
        combine(0, 0)
        combine(1, 1)
        reduce_chunk(1, 0, 1)
        combine(0, 1)

    @pl.when(core == 0)
    def _():
        for h in range(2):
            remote(ovf.at[h], ovf.at[h], ovf_ss.at[h], ovf_rs.at[0, 0, 0], peer).wait_send()
    for p in range(2):
        remote(ysend.at[p], ysend.at[p], y_ss.at[p], y_rs.at[0, 0, 0], peer).wait_send()
    ret_rest = tok_peer.at[pl.ds(quarter, 3 * quarter)]
    remote(ret_rest, ret_rest, ret_ss, ret_rs.at[0, 0], peer).wait_send()


def solution(mesh):
    n_ep, n_tp = mesh.shape['ep'], mesh.shape['tp']
    assert n_ep == 4 and n_tp == 2
    row_spec = P(('dp', 'ep', 'tp'), None)

    def local_moe(tokens, expert_ids, gate_vals, w_up, w_down):
        n_tok, hidden = tokens.shape
        n_loc, _, ffn = w_up.shape
        cap = capacity(n_tok, 1, n_loc * n_ep)
        pad = (cap + 15) // 16 * 16
        dims = (n_tok, hidden, ffn, n_loc, cap, pad)
        quarter = n_tok // 4
        col_slots = 2 * n_loc * cap
        n_ovf = col_slots - 2 * quarter
        f32, bf16 = jnp.float32, jnp.bfloat16
        dma = pltpu.SemaphoreType.DMA
        vmem = pl.BlockSpec(memory_space=pltpu.VMEM)
        hbm = pl.BlockSpec(memory_space=pl.ANY)
        picked = pl.pallas_call(
            functools.partial(moe_kernel, dims),
            out_shape=jax.ShapeDtypeStruct((n_tok, hidden), bf16),
            in_specs=[hbm, hbm, hbm, hbm],
            out_specs=vmem,
            scratch_shapes=[
                pltpu.VMEM((n_tok, hidden), bf16),
                pltpu.VMEM((n_tok, hidden), bf16),
                pltpu.VMEM((1, n_tok), jnp.int32),
                pltpu.VMEM((1, n_tok), jnp.int32),
                pltpu.VMEM((1, n_tok), f32),
                pltpu.VMEM((1, n_tok), f32),
                pltpu.VMEM((n_tok, 1), f32),
                pltpu.VMEM((8, 4 * n_loc, 128), f32),
                pltpu.VMEM((2, n_loc, 3, pad, hidden), bf16),
                pltpu.VMEM((2, n_loc, 4, pad, hidden), bf16),
                pltpu.VMEM((W_SLOTS, hidden, ffn), bf16),
                pltpu.VMEM((W_SLOTS, ffn, hidden), bf16),
                pltpu.VMEM((4 * pad, ffn), bf16),
                pltpu.VMEM((4, col_slots, hidden), f32),
                pltpu.VMEM((3 * col_slots, hidden), bf16),
                pltpu.VMEM((2, 2, quarter, hidden), f32),
                pltpu.VMEM((2, 2, quarter, hidden), f32),
                pltpu.VMEM((2, 2, quarter, hidden), f32),
                pltpu.VMEM((2, 2, 2, n_ovf, hidden), f32),
                pltpu.VMEM((n_tok, hidden), bf16),
                dma, dma, dma((W_SLOTS, 2, 2)), dma, dma, dma((2,)), dma((2,)), dma, dma,
                dma((2,)), dma((2, n_loc)), dma((2, 2)), dma((2, 2)), dma((2,)), dma((2, 2, 2)),
                dma((2,)), dma((2, 2, 2)), dma, dma((4, 2)),
                pltpu.SemaphoreType.REGULAR,
                pltpu.SemaphoreType.REGULAR,
            ],
            compiler_params=pltpu.CompilerParams(collective_id=0, has_side_effects=True, vmem_limit_bytes=VMEM_MIB << 20),
            name='moe_kernel',
        )(tokens, pltpu.with_memory_space_constraint(expert_ids.reshape(1, n_tok), pltpu.HBM), w_up, w_down)
        return (gate_vals * picked.astype(f32)).astype(bf16)

    return jax.shard_map(local_moe, mesh=mesh,
                         in_specs=(row_spec, row_spec, row_spec, P('ep', None, 'tp'), P('ep', 'tp', None)),
                         out_specs=row_spec, check_vma=False)
```

```python
import functools

import jax
import jax.numpy as jnp
from jax import lax
from jax.experimental import pallas as pl
from jax.experimental.pallas import tpu as pltpu
from jax.sharding import PartitionSpec as P

MESH = pl.DeviceIdType.MESH
W_SLOTS = 2
VMEM_MIB = 52


def capacity(tok_count, n_top, n_exp):
    return ((5 * tok_count * n_top) // (4 * n_exp) + 7) // 8 * 8


def moe_kernel(dims, tok_hbm, ids_hbm, up_hbm, down_hbm, out_ref,
               tok_own, tok_peer, ids_ref, ids_peer, slot_own, slot_peer, idx_col, cnts,
               send_rows, rows, up_buf, down_buf, hid, part, terms,
               ysend, arrived, mine, ovf, ret_recv,
               tok_sem, ids_sem, w_sem, ids_ss, ids_rs, ytok_ss, ytok_rs, cnt_ss, cnt_rs, disp_ss, disp_rs,
               d2d_ss, d2d_rs, ovf_ss, ovf_rs, y_ss, y_rs, ret_ss, ret_rs, go_sem, part_free):
    n_tok, hidden, ffn, n_loc, cap, pad = dims
    n_exp = 4 * n_loc
    col_exp = 2 * n_loc
    col_slots = col_exp * cap
    region = n_tok // 2
    quarter = region // 2
    chunk = quarter // 2
    n_ovf = col_slots - region
    f32, bf16, i32 = jnp.float32, jnp.bfloat16, jnp.int32
    dp, tp, ep = lax.axis_index('dp'), lax.axis_index('tp'), lax.axis_index('ep')
    core = lax.rem(ep, 2)
    col = ep // 2
    iota = functools.partial(lax.broadcasted_iota, i32)

    def rel_ep(d):
        flipped = lax.rem(ep + 2 * (d // 2), 4)
        return flipped + (d % 2) * (1 - 2 * lax.rem(flipped, 2))

    def dev(d, h=0):
        return (dp, tp if h == 0 else 1 - tp, rel_ep(d))

    peer = dev(0, 1)
    partner = dev(1)
    others = [(h, d) for d in range(4) for h in range(2) if (h, d) != (0, 0)]

    def remote(src, dst, ss, rs, target):
        return pltpu.make_async_remote_copy(src, dst, ss, rs, device_id=target, device_id_type=MESH)

    def parity(g):
        return lax.rem(g + core, 2)

    def w_copies(n):
        slot, e = lax.rem(n, W_SLOTS), lax.rem(n, n_loc)
        halves = []
        for i, (src, dst) in enumerate(((up_hbm, up_buf), (down_hbm, down_buf))):
            size = src.shape[1] // 2
            halves.append([pltpu.make_async_copy(src.at[e, pl.ds(m * size, size)], dst.at[slot, pl.ds(m * size, size)],
                                                 w_sem.at[slot, i, m]) for m in range(2)])
        return halves

    def for_all(what, copies):
        for cp in copies:
            getattr(cp, what)()

    def w_start(n):
        for half in w_copies(n):
            for cp in half:
                cp.start()

    tok_cp = pltpu.make_async_copy(tok_hbm, tok_own, tok_sem)
    tok_cp.start()
    ids_load = pltpu.make_async_copy(ids_hbm, ids_ref, ids_sem)
    ids_load.start()

    barrier = pltpu.get_barrier_semaphore()
    for h, d in others:
        pl.semaphore_signal(barrier, inc=1, device_id=dev(d, h), device_id_type=MESH)
    pl.semaphore_wait(barrier, len(others))

    ids_load.wait()
    ids_cp = remote(ids_ref, ids_peer, ids_ss, ids_rs, peer)
    ids_cp.start()
    tok_cp.wait()

    half_tok = n_tok // 2
    cut = n_tok * 31 // 32
    ytok = [remote(tok_own.at[pl.ds(a, n)], tok_peer.at[pl.ds(a, n)], ytok_ss.at[i], ytok_rs.at[i], peer)
            for i, (a, n) in enumerate(((0, half_tok), (half_tok, cut - half_tok), (cut, n_tok - cut)))]

    @pl.when(core == 0)
    def _():
        for cp in ytok:
            cp.start()

    for n in range(W_SLOTS):
        w_start(n)

    lane = 128
    tri = (iota((lane, lane), 0) < iota((lane, lane), 1)).astype(bf16)
    eye = iota((lane, lane), 0) == iota((lane, lane), 1)
    exp_iota = iota((n_exp, lane), 0)
    row_e, col_e = iota((n_exp, n_exp), 0), iota((n_exp, n_exp), 1)
    before_in_col = ((col_e < row_e) & (col_e // col_exp == row_e // col_exp)).astype(bf16)

    def hits(ids, b):
        id_row = ids[:, pl.ds(b * lane, lane)]
        return id_row, jnp.where(exp_iota == id_row, 1.0, 0.0).astype(f32)

    def route(ids, slots):
        counts = jnp.zeros((n_exp, 1), f32)
        for b in range(n_tok // lane):
            id_row, hit = hits(ids, b)
            before = jnp.dot(hit.astype(bf16), tri, preferred_element_type=f32) + counts
            rank = jnp.sum(hit * before, axis=0, keepdims=True)
            counts = counts + jnp.sum(hit, axis=1, keepdims=True)
            slots[:, pl.ds(b * lane, lane)] = jnp.where(rank < cap, id_row.astype(f32) * cap + rank, -1.0)
        return counts

    def cnt_copy(h, d):
        return remote(cnts.at[0], cnts.at[4 * h + d], cnt_ss, cnt_rs, dev(d, h))

    kept = jnp.minimum(route(ids_ref, slot_own), float(cap))
    kept = jnp.broadcast_to(kept, (n_exp, lane))
    cnts[0] = kept

    def disp_copy(h, e, d):
        return remote(send_rows.at[h, e, d - 1, pl.ds(0, cap)], rows.at[d % 2, e, 2 * h + d // 2, pl.ds(0, cap)],
                      disp_ss.at[h], disp_rs.at[d % 2, e], dev(d))

    def disp_start(h, e):
        for d in (2, 3, 1):
            disp_copy(h, e, d).start()

    def dispatch(h, stage=0):
        slots, toks = (slot_own, tok_own) if h == 0 else (slot_peer, tok_peer)

        def step(e2, carry):
            k_iota = iota((cap, 1), 0)
            pair = [(2 * e2 + m, d) for m in range(2) for d in range(4)]
            target = jnp.concatenate([(k_iota + (rel_ep(d) * n_loc + e) * cap).astype(f32) for e, d in pair], axis=0)
            span = [pl.ds(0, n_tok), pl.ds(0, half_tok), pl.ds(half_tok, half_tok)][stage]
            pick = jnp.where(slots[:, span] == target, 1.0, 0.0).astype(bf16)
            picked = jnp.dot(pick, toks[span, :], preferred_element_type=f32)
            if stage == 1:
                part[e2, pl.ds(0, 8 * cap)] = picked
                return carry
            if stage == 2:
                picked = picked + part[e2, pl.ds(0, 8 * cap)]
            for m, (e, d) in enumerate(pair):
                block = picked[m * cap:(m + 1) * cap].astype(bf16)
                if d == 0:
                    rows[0, e, 2 * h, pl.ds(0, cap)] = block
                else:
                    send_rows[h, e, d - 1, pl.ds(0, cap)] = block
            for m in range(2):
                if h == 1:
                    disp_start(h, 2 * e2 + m)
                else:
                    @pl.when((core == 0) | (e2 < n_loc // 4))
                    def _():
                        disp_start(h, 2 * e2 + m)
            return carry

        lax.fori_loop(0, n_loc // 2, step, 0)

    dispatch(0)

    for h, d in others:
        cnt_copy(h, d).start()

    first_row = jnp.dot(before_in_col, kept.astype(bf16), preferred_element_type=f32)
    for b in range(n_tok // lane):
        here = pl.ds(b * lane, lane)
        id_row, hit = hits(ids_ref, b)
        slot = slot_own[:, here]
        rank = slot - id_row.astype(f32) * cap
        joint = (jnp.sum(hit * first_row, axis=0, keepdims=True) + rank).astype(i32)
        home = id_row // col_exp
        stays = joint < region
        where_col = jnp.where(stays, home, 1 - home)
        q = jnp.where(stays, joint, 2 * region - 1 - joint)
        idx = lax.rem(q // chunk, 2) * region + (2 * where_col + q // quarter) * chunk + lax.rem(q, chunk)
        idx = jnp.where(slot < 0.0, -1.0, idx.astype(f32))
        idx_col[here, :] = jnp.sum(jnp.where(eye, idx, 0.0), axis=1, keepdims=True)

    ids_cp.wait_recv()
    route(ids_peer, slot_peer)

    @pl.when(core == 0)
    def _():
        ytok[0].wait_recv()
        dispatch(1, 1)
        ytok[0].wait_send()
        ytok[1].wait_send()
        pl.semaphore_signal(go_sem, inc=1, device_id=partner, device_id_type=MESH)

    @pl.when(core == 1)
    def _():
        pl.semaphore_wait(go_sem, 1)
        for cp in ytok:
            cp.start()

    def d2d_copy(h, g, e):
        here = pl.ds(pl.multiple_of((core * n_loc + e) * cap, 8), cap)
        half = pl.ds(2 * h, 2)
        return remote(part.at[half, here], part.at[half, here], d2d_ss.at[h, g], d2d_rs.at[h, g], partner)

    def experts(g, extra):
        p = parity(g)

        def arrival(e, blocks):
            here = rows.at[p, e, pl.ds(0, blocks), pl.ds(0, cap)]
            remote(here, here, disp_ss.at[0], disp_rs.at[p, e], peer).wait_recv()

        def step(e, carry):
            n = g * n_loc + e
            slot = lax.rem(n, W_SLOTS)

            @pl.when(p == 1)
            def _():
                arrival(e, 4)

            @pl.when(p == 0)
            def _():
                arrival(e, 2)
            ups, downs = w_copies(n)
            for_all('wait', ups)
            x = rows[p, e].reshape(4 * pad, hidden)
            width = 512
            for j in range(ffn // width):
                cols = pl.ds(j * width, width)
                pre = jnp.dot(x, up_buf[slot, :, cols], preferred_element_type=f32)
                hid[:, cols] = jax.nn.gelu(pre, approximate=True).astype(bf16)

            @pl.when(n + W_SLOTS < 2 * n_loc)
            def _():
                for_all('start', w_copies(n + W_SLOTS)[0])
            for_all('wait', downs)
            res = jnp.dot(hid[...], down_buf[slot], preferred_element_type=f32)
            here = pl.ds(pl.multiple_of((core * n_loc + e) * cap, 8), cap)
            for hk in range(4):
                part[hk, here] = res[hk * pad:hk * pad + cap]
            d2d_copy(1, g, e).start()
            d2d_copy(0, g, e).start()

            @pl.when(n + W_SLOTS < 2 * n_loc)
            def _():
                for_all('start', w_copies(n + W_SLOTS)[1])
            extra(e)
            return carry

        lax.fori_loop(0, n_loc, step, 0)

    slot_iota = iota((1, col_slots), 1)
    slot_exp, slot_rank = slot_iota // cap, lax.rem(slot_iota, cap)
    exp_match = iota((col_exp, col_slots), 0) == slot_exp
    before_exp = (iota((col_exp, col_exp), 1) < iota((col_exp, col_exp), 0)).astype(bf16)

    def positions(h, p, k):
        cnt = cnts[4 * h + p + 2 * k, pl.ds(pl.multiple_of(col * col_exp, 8), col_exp), :]
        start = jnp.dot(before_exp, cnt.astype(bf16), preferred_element_type=f32)
        start_row = jnp.sum(jnp.where(exp_match, start[:, 0:1], 0.0), axis=0, keepdims=True)
        cnt_row = jnp.sum(jnp.where(exp_match, cnt[:, 0:1], 0.0), axis=0, keepdims=True)
        rank = slot_rank.astype(f32)
        return jnp.where(rank < cnt_row, start_row + rank, -1.0)

    def ovf_copy(h, g, k):
        p = parity(g)
        return remote(ovf.at[h, p, k], ovf.at[h, 1 - p, 1 - k], ovf_ss.at[h], ovf_rs.at[h, g, 1 - k], dev(3))

    def y_copy(p, k, i):
        here = pl.ds(i * chunk, chunk)
        return remote(ysend.at[p, k, here], arrived.at[p, k, here], y_ss.at[p], y_rs.at[p, k, i], peer)

    def split(block, half):
        start = pl.multiple_of(half * half_col, 64)
        x = part[block, pl.ds(start, half_col)]
        hi = x.astype(bf16)
        rest = x - hi.astype(f32)
        mid = rest.astype(bf16)
        low = (rest - mid.astype(f32)).astype(bf16)
        for t, term in enumerate((hi, mid, low)):
            terms[pl.ds(pl.multiple_of(start + t * col_slots, 64), half_col)] = term

    def compact(h, g):
        p = parity(g)
        dest = ysend if h == 1 else mine

        for k in (1, 0):
            where = positions(h, p, k)
            split(2 * h + k, core)
            if k == 1:
                d2d_wait(h, g)
            split(2 * h + k, 1 - core)

            def take(target):
                pick = jnp.where(where == target.astype(f32), 1.0, 0.0).astype(bf16)
                return jnp.dot(jnp.concatenate([pick] * 3, axis=1), terms[...], preferred_element_type=f32)

            row = iota((quarter, 1), 0) + core * quarter

            early = h == 1 and g == 0 and k == 1
            if early:
                dest[p, k, pl.ds(0, chunk)] = take(row[0:chunk])
                y_copy(p, k, 0).start()

            @pl.when(core == 0)
            def _():
                if early:
                    got = take(jnp.concatenate([row[chunk:], (col_slots - 1) - iota((n_ovf, 1), 0)], axis=0))
                    dest[p, k, pl.ds(chunk, chunk)] = got[0:chunk]
                    ovf[h, p, k] = got[chunk:chunk + n_ovf]
                    y_copy(p, k, 1).start()
                    ovf_copy(h, g, k).start()
                    return
                got = take(jnp.concatenate([row, (col_slots - 1) - iota((n_ovf, 1), 0)], axis=0))
                dest[p, k] = got[0:quarter]
                ovf[h, p, k] = got[quarter:quarter + n_ovf]
                if h == 1:
                    y_copy(p, k, 0).start()
                    y_copy(p, k, 1).start()
                    ovf_copy(h, g, k).start()

            @pl.when(core == 1)
            def _():
                if early:
                    dest[p, k, pl.ds(chunk, chunk)] = take(row[chunk:])
                    return
                dest[p, k] = take(row)
                if h == 1 and (g == 0 or k == 1):
                    y_copy(p, k, 0).start()

    def ovf_start(h, g):
        for k in (1, 0):
            ovf_copy(h, g, k).start()

    half_col = n_loc * cap

    def d2d_all(h, g):
        here = part.at[pl.ds(2 * h, 2), pl.ds(0, half_col)]
        return remote(here, here, d2d_ss.at[h, g], d2d_rs.at[h, g], partner)

    def d2d_wait(h, g):
        d2d_all(h, g).wait_recv()

    def d2d_drain(g):
        for h in range(2):
            d2d_all(h, g).wait_send()

    def fill(h, g):
        p = parity(g)
        dest = ysend if h == 1 else mine

        @pl.when(core == 1)
        def _():
            for k in (1, 0):
                here = pl.ds(quarter - n_ovf, n_ovf)
                ovf_copy(h, g, 1 - k).wait_recv()
                dest[p, k, here] = dest[p, k, here] + ovf[h, p, k]
                if h == 1:
                    if g == 1 and k == 0:
                        y_copy(p, k, 0).start()
                    y_copy(p, k, 1).start()

    def ret_rows(p, k, i):
        start = (2 * p + k) * quarter + i * chunk
        return tok_peer.at[pl.ds(pl.multiple_of(start, chunk), chunk)]

    def ret_copy(p, k, i):
        d = p + 2 * k
        there = pl.ds(pl.multiple_of(i * region + ep * chunk, chunk), chunk)
        return remote(ret_rows(p, k, i), ret_recv.at[there], ret_ss, ret_rs.at[d, i], dev(d))

    def ret_wait(d, i):
        remote(tok_peer.at[pl.ds(0, chunk)], ret_recv.at[pl.ds(0, chunk)], ret_ss, ret_rs.at[d, i],
               peer).wait_recv()

    def reduce_chunk(g, k, i):
        p = parity(g)
        here = pl.ds(i * chunk, chunk)
        y_copy(p, k, i).wait_recv()
        total = (mine[p, k, here] + arrived[p, k, here]).astype(bf16)
        if k == 1:
            ret_rows(p, k, i)[...] = total
            ret_copy(p, k, i).start()
        else:
            @pl.when(p == 0)
            def _():
                ret_recv[pl.ds(pl.multiple_of(i * region + ep * chunk, chunk), chunk)] = total

            @pl.when(p == 1)
            def _():
                ret_rows(p, k, i)[...] = total
                ret_copy(p, k, i).start()

    out_rows = 256

    def combine(far, i, first=False):
        for d in ((2, 3) if far else (1,)):
            ret_wait(d, i)
        start = i * region + (lax.rem(col + far, 2)) * 2 * chunk
        here_r = pl.ds(pl.multiple_of(start, chunk), 2 * chunk)
        target = (iota((1, 2 * chunk), 1) + start).astype(f32)

        for j in range(n_tok // out_rows):
            here = pl.ds(j * out_rows, out_rows)
            pick = jnp.where(idx_col[here, :] == target, 1.0, 0.0).astype(bf16)
            got = jnp.dot(pick, ret_recv[here_r, :], preferred_element_type=f32)
            if first:
                out_ref[here, :] = got.astype(bf16)
            else:
                out_ref[here, :] = (out_ref[here, :].astype(f32) + got).astype(bf16)

    @pl.when(core == 0)
    def _():
        for cp in ytok[1:]:
            cp.wait_recv()
        dispatch(1, 2)

    def during_b(e):
        @pl.when(e == n_loc // 2)
        def _():
            fill(1, 0)

            @pl.when(core == 0)
            def _():
                ovf_start(0, 0)

    cnt_all = remote(cnts.at[pl.ds(1, 7)], cnts.at[pl.ds(1, 7)], cnt_ss, cnt_rs, peer)
    cnt_all.wait_recv()
    experts(0, lambda e: None)

    @pl.when(core == 1)
    def _():
        for e in range(n_loc // 2, n_loc):
            disp_start(0, e)
    compact(1, 0)

    @pl.when(core == 1)
    def _():
        for cp in ytok:
            cp.wait_recv()
        dispatch(1)
    compact(0, 0)
    pl.semaphore_signal(part_free, inc=1, device_id=partner, device_id_type=MESH)
    pl.semaphore_wait(part_free, 1)

    d2d_drain(0)
    experts(1, during_b)
    compact(1, 1)
    compact(0, 1)

    @pl.when(core == 0)
    def _():
        ovf_start(0, 1)
        for k, i in ((1, 0), (1, 1), (0, 0), (0, 1)):
            reduce_chunk(0, k, i)

    @pl.when(core == 1)
    def _():
        fill(0, 0)
        for k, i in ((1, 0), (0, 0), (1, 1)):
            reduce_chunk(0, k, i)
        fill(1, 1)
        reduce_chunk(0, 0, 1)

    ids_cp.wait_send()

    @pl.when(core == 1)
    def _():
        ytok[0].wait_send()
        ytok[1].wait_send()
    ytok[2].wait_send()
    cnt_all.wait_send()

    for h in range(2):
        sent = send_rows.at[h, :, :, pl.ds(0, cap)]
        remote(sent, sent, disp_ss.at[h], disp_rs.at[0, 0], peer).wait_send()
    d2d_drain(1)

    @pl.when(core == 0)
    def _():
        reduce_chunk(1, 1, 0)
        reduce_chunk(1, 1, 1)
        combine(1, 0, True)
        combine(0, 0)
        combine(1, 1)
        combine(0, 1)
        reduce_chunk(1, 0, 0)
        reduce_chunk(1, 0, 1)

    @pl.when(core == 1)
    def _():
        reduce_chunk(1, 1, 0)
        fill(0, 1)
        combine(1, 0, True)
        reduce_chunk(1, 1, 1)
        reduce_chunk(1, 0, 0)
        combine(0, 0)
        combine(1, 1)
        reduce_chunk(1, 0, 1)
        combine(0, 1)

    @pl.when(core == 0)
    def _():
        for h in range(2):
            remote(ovf.at[h], ovf.at[h], ovf_ss.at[h], ovf_rs.at[0, 0, 0], peer).wait_send()
    for p in range(2):
        remote(ysend.at[p], ysend.at[p], y_ss.at[p], y_rs.at[0, 0, 0], peer).wait_send()
    ret_rest = tok_peer.at[pl.ds(quarter, 3 * quarter)]
    remote(ret_rest, ret_rest, ret_ss, ret_rs.at[0, 0], peer).wait_send()


def solution(mesh):
    n_ep, n_tp = mesh.shape['ep'], mesh.shape['tp']
    assert n_ep == 4 and n_tp == 2
    row_spec = P(('dp', 'ep', 'tp'), None)

    def local_moe(tokens, expert_ids, gate_vals, w_up, w_down):
        n_tok, hidden = tokens.shape
        n_loc, _, ffn = w_up.shape
        cap = capacity(n_tok, 1, n_loc * n_ep)
        pad = (cap + 15) // 16 * 16
        dims = (n_tok, hidden, ffn, n_loc, cap, pad)
        quarter = n_tok // 4
        col_slots = 2 * n_loc * cap
        n_ovf = col_slots - 2 * quarter
        f32, bf16 = jnp.float32, jnp.bfloat16
        dma = pltpu.SemaphoreType.DMA
        vmem = pl.BlockSpec(memory_space=pltpu.VMEM)
        hbm = pl.BlockSpec(memory_space=pl.ANY)
        picked = pl.pallas_call(
            functools.partial(moe_kernel, dims),
            out_shape=jax.ShapeDtypeStruct((n_tok, hidden), bf16),
            in_specs=[hbm, hbm, hbm, hbm],
            out_specs=vmem,
            scratch_shapes=[
                pltpu.VMEM((n_tok, hidden), bf16),
                pltpu.VMEM((n_tok, hidden), bf16),
                pltpu.VMEM((1, n_tok), jnp.int32),
                pltpu.VMEM((1, n_tok), jnp.int32),
                pltpu.VMEM((1, n_tok), f32),
                pltpu.VMEM((1, n_tok), f32),
                pltpu.VMEM((n_tok, 1), f32),
                pltpu.VMEM((8, 4 * n_loc, 128), f32),
                pltpu.VMEM((2, n_loc, 3, pad, hidden), bf16),
                pltpu.VMEM((2, n_loc, 4, pad, hidden), bf16),
                pltpu.VMEM((W_SLOTS, hidden, ffn), bf16),
                pltpu.VMEM((W_SLOTS, ffn, hidden), bf16),
                pltpu.VMEM((4 * pad, ffn), bf16),
                pltpu.VMEM((4, col_slots, hidden), f32),
                pltpu.VMEM((3 * col_slots, hidden), bf16),
                pltpu.VMEM((2, 2, quarter, hidden), f32),
                pltpu.VMEM((2, 2, quarter, hidden), f32),
                pltpu.VMEM((2, 2, quarter, hidden), f32),
                pltpu.VMEM((2, 2, 2, n_ovf, hidden), f32),
                pltpu.VMEM((n_tok, hidden), bf16),
                dma, dma, dma((W_SLOTS, 2, 2)), dma, dma, dma((3,)), dma((3,)), dma, dma,
                dma((2,)), dma((2, n_loc)), dma((2, 2)), dma((2, 2)), dma((2,)), dma((2, 2, 2)),
                dma((2,)), dma((2, 2, 2)), dma, dma((4, 2)),
                pltpu.SemaphoreType.REGULAR,
                pltpu.SemaphoreType.REGULAR,
            ],
            compiler_params=pltpu.CompilerParams(collective_id=0, has_side_effects=True, vmem_limit_bytes=VMEM_MIB << 20),
            name='moe_kernel',
        )(tokens, pltpu.with_memory_space_constraint(expert_ids.reshape(1, n_tok), pltpu.HBM), w_up, w_down)
        return (gate_vals * picked.astype(f32)).astype(bf16)

    return jax.shard_map(local_moe, mesh=mesh,
                         in_specs=(row_spec, row_spec, row_spec, P('ep', None, 'tp'), P('ep', 'tp', None)),
                         out_specs=row_spec, check_vma=False)
```

```python
import functools

import jax
import jax.numpy as jnp
from jax import lax
from jax.experimental import pallas as pl
from jax.experimental.pallas import tpu as pltpu
from jax.sharding import PartitionSpec as P

MESH = pl.DeviceIdType.MESH
W_SLOTS = 2
VMEM_MIB = 52


def capacity(tok_count, n_top, n_exp):
    return ((5 * tok_count * n_top) // (4 * n_exp) + 7) // 8 * 8


def moe_kernel(dims, tok_hbm, ids_hbm, up_hbm, down_hbm, out_ref,
               tok_own, tok_peer, ids_ref, ids_peer, slot_own, slot_peer, idx_col, cnts,
               send_rows, rows, up_buf, down_buf, hid, part, terms,
               ysend, arrived, mine, ovf, ret_recv,
               tok_sem, ids_sem, w_sem, ids_ss, ids_rs, ytok_ss, ytok_rs, cnt_ss, cnt_rs, disp_ss, disp_rs,
               d2d_ss, d2d_rs, ovf_ss, ovf_rs, y_ss, y_rs, ret_ss, ret_rs, go_sem, part_free):
    n_tok, hidden, ffn, n_loc, cap, pad = dims
    n_exp = 4 * n_loc
    col_exp = 2 * n_loc
    col_slots = col_exp * cap
    region = n_tok // 2
    quarter = region // 2
    chunk = quarter // 2
    n_ovf = col_slots - region
    f32, bf16, i32 = jnp.float32, jnp.bfloat16, jnp.int32
    dp, tp, ep = lax.axis_index('dp'), lax.axis_index('tp'), lax.axis_index('ep')
    core = lax.rem(ep, 2)
    col = ep // 2
    iota = functools.partial(lax.broadcasted_iota, i32)

    def rel_ep(d):
        flipped = lax.rem(ep + 2 * (d // 2), 4)
        return flipped + (d % 2) * (1 - 2 * lax.rem(flipped, 2))

    def dev(d, h=0):
        return (dp, tp if h == 0 else 1 - tp, rel_ep(d))

    peer = dev(0, 1)
    partner = dev(1)
    others = [(h, d) for d in range(4) for h in range(2) if (h, d) != (0, 0)]

    def remote(src, dst, ss, rs, target):
        return pltpu.make_async_remote_copy(src, dst, ss, rs, device_id=target, device_id_type=MESH)

    def parity(g):
        return lax.rem(g + core, 2)

    def w_copies(n):
        slot, e = lax.rem(n, W_SLOTS), lax.rem(n, n_loc)
        halves = []
        for i, (src, dst) in enumerate(((up_hbm, up_buf), (down_hbm, down_buf))):
            size = src.shape[1] // 2
            halves.append([pltpu.make_async_copy(src.at[e, pl.ds(m * size, size)], dst.at[slot, pl.ds(m * size, size)],
                                                 w_sem.at[slot, i, m]) for m in range(2)])
        return halves

    def for_all(what, copies):
        for cp in copies:
            getattr(cp, what)()

    def w_start(n):
        for half in w_copies(n):
            for cp in half:
                cp.start()

    tok_cp = pltpu.make_async_copy(tok_hbm, tok_own, tok_sem)
    tok_cp.start()
    ids_load = pltpu.make_async_copy(ids_hbm, ids_ref, ids_sem)
    ids_load.start()

    barrier = pltpu.get_barrier_semaphore()
    for h, d in others:
        pl.semaphore_signal(barrier, inc=1, device_id=dev(d, h), device_id_type=MESH)
    pl.semaphore_wait(barrier, len(others))

    ids_load.wait()
    ids_cp = remote(ids_ref, ids_peer, ids_ss, ids_rs, peer)
    ids_cp.start()
    tok_cp.wait()

    half_tok = n_tok // 2
    cut = n_tok * 31 // 32
    ytok = [remote(tok_own.at[pl.ds(a, n)], tok_peer.at[pl.ds(a, n)], ytok_ss.at[i], ytok_rs.at[i], peer)
            for i, (a, n) in enumerate(((0, half_tok), (half_tok, cut - half_tok), (cut, n_tok - cut)))]

    @pl.when(core == 0)
    def _():
        for cp in ytok:
            cp.start()

    for n in range(W_SLOTS):
        w_start(n)

    lane = 128
    tri = (iota((lane, lane), 0) < iota((lane, lane), 1)).astype(bf16)
    eye = iota((lane, lane), 0) == iota((lane, lane), 1)
    exp_iota = iota((n_exp, lane), 0)
    row_e, col_e = iota((n_exp, n_exp), 0), iota((n_exp, n_exp), 1)
    before_in_col = ((col_e < row_e) & (col_e // col_exp == row_e // col_exp)).astype(bf16)

    def hits(ids, b):
        id_row = ids[:, pl.ds(b * lane, lane)]
        return id_row, jnp.where(exp_iota == id_row, 1.0, 0.0).astype(f32)

    def route(ids, slots):
        counts = jnp.zeros((n_exp, 1), f32)
        for b in range(n_tok // lane):
            id_row, hit = hits(ids, b)
            before = jnp.dot(hit.astype(bf16), tri, preferred_element_type=f32) + counts
            rank = jnp.sum(hit * before, axis=0, keepdims=True)
            counts = counts + jnp.sum(hit, axis=1, keepdims=True)
            slots[:, pl.ds(b * lane, lane)] = jnp.where(rank < cap, id_row.astype(f32) * cap + rank, -1.0)
        return counts

    def cnt_copy(h, d):
        return remote(cnts.at[0], cnts.at[4 * h + d], cnt_ss, cnt_rs, dev(d, h))

    kept = jnp.minimum(route(ids_ref, slot_own), float(cap))
    kept = jnp.broadcast_to(kept, (n_exp, lane))
    cnts[0] = kept

    def disp_copy(h, e, d):
        return remote(send_rows.at[h, e, d - 1, pl.ds(0, cap)], rows.at[d % 2, e, 2 * h + d // 2, pl.ds(0, cap)],
                      disp_ss.at[h], disp_rs.at[d % 2, e], dev(d))

    def disp_start(h, e):
        for d in (2, 3, 1):
            disp_copy(h, e, d).start()

    def dispatch(h, stage=0):
        slots, toks = (slot_own, tok_own) if h == 0 else (slot_peer, tok_peer)

        def step(e2, carry):
            k_iota = iota((cap, 1), 0)
            pair = [(2 * e2 + m, d) for m in range(2) for d in range(4)]
            target = jnp.concatenate([(k_iota + (rel_ep(d) * n_loc + e) * cap).astype(f32) for e, d in pair], axis=0)
            span = [pl.ds(0, n_tok), pl.ds(0, half_tok), pl.ds(half_tok, half_tok)][stage]
            pick = jnp.where(slots[:, span] == target, 1.0, 0.0).astype(bf16)
            picked = jnp.dot(pick, toks[span, :], preferred_element_type=f32)
            if stage == 1:
                part[e2, pl.ds(0, 8 * cap)] = picked
                return carry
            if stage == 2:
                picked = picked + part[e2, pl.ds(0, 8 * cap)]
            for m, (e, d) in enumerate(pair):
                block = picked[m * cap:(m + 1) * cap].astype(bf16)
                if d == 0:
                    rows[0, e, 2 * h, pl.ds(0, cap)] = block
                else:
                    send_rows[h, e, d - 1, pl.ds(0, cap)] = block
            for m in range(2):
                if h == 1:
                    disp_start(h, 2 * e2 + m)
                else:
                    @pl.when((core == 0) | (e2 < n_loc // 4))
                    def _():
                        disp_start(h, 2 * e2 + m)
            return carry

        lax.fori_loop(0, n_loc // 2, step, 0)

    dispatch(0)

    for h, d in others:
        cnt_copy(h, d).start()

    first_row = jnp.dot(before_in_col, kept.astype(bf16), preferred_element_type=f32)
    for b in range(n_tok // lane):
        here = pl.ds(b * lane, lane)
        id_row, hit = hits(ids_ref, b)
        slot = slot_own[:, here]
        rank = slot - id_row.astype(f32) * cap
        joint = (jnp.sum(hit * first_row, axis=0, keepdims=True) + rank).astype(i32)
        home = id_row // col_exp
        stays = joint < region
        where_col = jnp.where(stays, home, 1 - home)
        q = jnp.where(stays, joint, 2 * region - 1 - joint)
        idx = lax.rem(q // chunk, 2) * region + (2 * where_col + q // quarter) * chunk + lax.rem(q, chunk)
        idx = jnp.where(slot < 0.0, -1.0, idx.astype(f32))
        idx_col[here, :] = jnp.sum(jnp.where(eye, idx, 0.0), axis=1, keepdims=True)

    ids_cp.wait_recv()
    route(ids_peer, slot_peer)

    @pl.when(core == 0)
    def _():
        ytok[0].wait_recv()
        dispatch(1, 1)
        for cp in ytok:
            cp.wait_send()
        pl.semaphore_signal(go_sem, inc=1, device_id=partner, device_id_type=MESH)

    @pl.when(core == 1)
    def _():
        pl.semaphore_wait(go_sem, 1)
        for cp in ytok:
            cp.start()

    def d2d_copy(h, g, e):
        here = pl.ds(pl.multiple_of((core * n_loc + e) * cap, 8), cap)
        half = pl.ds(2 * h, 2)
        return remote(part.at[half, here], part.at[half, here], d2d_ss.at[h, g], d2d_rs.at[h, g], partner)

    def experts(g, extra):
        p = parity(g)

        def arrival(e, blocks):
            here = rows.at[p, e, pl.ds(0, blocks), pl.ds(0, cap)]
            remote(here, here, disp_ss.at[0], disp_rs.at[p, e], peer).wait_recv()

        def step(e, carry):
            n = g * n_loc + e
            slot = lax.rem(n, W_SLOTS)

            @pl.when(p == 1)
            def _():
                arrival(e, 4)

            @pl.when(p == 0)
            def _():
                arrival(e, 2)
            ups, downs = w_copies(n)
            for_all('wait', ups)
            x = rows[p, e].reshape(4 * pad, hidden)
            width = 512
            for j in range(ffn // width):
                cols = pl.ds(j * width, width)
                pre = jnp.dot(x, up_buf[slot, :, cols], preferred_element_type=f32)
                hid[:, cols] = jax.nn.gelu(pre, approximate=True).astype(bf16)

            @pl.when(n + W_SLOTS < 2 * n_loc)
            def _():
                for_all('start', w_copies(n + W_SLOTS)[0])
            for_all('wait', downs)
            res = jnp.dot(hid[...], down_buf[slot], preferred_element_type=f32)
            here = pl.ds(pl.multiple_of((core * n_loc + e) * cap, 8), cap)
            for hk in range(4):
                part[hk, here] = res[hk * pad:hk * pad + cap]
            d2d_copy(1, g, e).start()
            d2d_copy(0, g, e).start()

            @pl.when(n + W_SLOTS < 2 * n_loc)
            def _():
                for_all('start', w_copies(n + W_SLOTS)[1])
            extra(e)
            return carry

        lax.fori_loop(0, n_loc, step, 0)

    slot_iota = iota((1, col_slots), 1)
    slot_exp, slot_rank = slot_iota // cap, lax.rem(slot_iota, cap)
    exp_match = iota((col_exp, col_slots), 0) == slot_exp
    before_exp = (iota((col_exp, col_exp), 1) < iota((col_exp, col_exp), 0)).astype(bf16)

    def positions(h, p, k):
        cnt = cnts[4 * h + p + 2 * k, pl.ds(pl.multiple_of(col * col_exp, 8), col_exp), :]
        start = jnp.dot(before_exp, cnt.astype(bf16), preferred_element_type=f32)
        start_row = jnp.sum(jnp.where(exp_match, start[:, 0:1], 0.0), axis=0, keepdims=True)
        cnt_row = jnp.sum(jnp.where(exp_match, cnt[:, 0:1], 0.0), axis=0, keepdims=True)
        rank = slot_rank.astype(f32)
        return jnp.where(rank < cnt_row, start_row + rank, -1.0)

    def ovf_copy(h, g, k):
        p = parity(g)
        return remote(ovf.at[h, p, k], ovf.at[h, 1 - p, 1 - k], ovf_ss.at[h], ovf_rs.at[h, g, 1 - k], dev(3))

    def y_copy(p, k, i):
        here = pl.ds(i * chunk, chunk)
        return remote(ysend.at[p, k, here], arrived.at[p, k, here], y_ss.at[p], y_rs.at[p, k, i], peer)

    def split(block, half):
        start = pl.multiple_of(half * half_col, 64)
        x = part[block, pl.ds(start, half_col)]
        hi = x.astype(bf16)
        rest = x - hi.astype(f32)
        mid = rest.astype(bf16)
        low = (rest - mid.astype(f32)).astype(bf16)
        for t, term in enumerate((hi, mid, low)):
            terms[pl.ds(pl.multiple_of(start + t * col_slots, 64), half_col)] = term

    def compact(h, g):
        p = parity(g)
        dest = ysend if h == 1 else mine

        for k in (1, 0):
            where = positions(h, p, k)
            split(2 * h + k, core)
            if k == 1:
                d2d_wait(h, g)
            split(2 * h + k, 1 - core)

            def take(target):
                pick = jnp.where(where == target.astype(f32), 1.0, 0.0).astype(bf16)
                return jnp.dot(jnp.concatenate([pick] * 3, axis=1), terms[...], preferred_element_type=f32)

            row = iota((quarter, 1), 0) + core * quarter

            early = h == 1 and g == 0 and k == 1
            if early:
                dest[p, k, pl.ds(0, chunk)] = take(row[0:chunk])
                y_copy(p, k, 0).start()

            @pl.when(core == 0)
            def _():
                if early:
                    got = take(jnp.concatenate([row[chunk:], (col_slots - 1) - iota((n_ovf, 1), 0)], axis=0))
                    dest[p, k, pl.ds(chunk, chunk)] = got[0:chunk]
                    ovf[h, p, k] = got[chunk:chunk + n_ovf]
                    y_copy(p, k, 1).start()
                    ovf_copy(h, g, k).start()
                    return
                got = take(jnp.concatenate([row, (col_slots - 1) - iota((n_ovf, 1), 0)], axis=0))
                dest[p, k] = got[0:quarter]
                ovf[h, p, k] = got[quarter:quarter + n_ovf]
                if h == 1:
                    y_copy(p, k, 0).start()
                    y_copy(p, k, 1).start()
                    ovf_copy(h, g, k).start()

            @pl.when(core == 1)
            def _():
                if early:
                    dest[p, k, pl.ds(chunk, chunk)] = take(row[chunk:])
                    return
                dest[p, k] = take(row)
                if h == 1 and (g == 0 or k == 1):
                    y_copy(p, k, 0).start()

    def ovf_start(h, g):
        for k in (1, 0):
            ovf_copy(h, g, k).start()

    half_col = n_loc * cap

    def d2d_all(h, g):
        here = part.at[pl.ds(2 * h, 2), pl.ds(0, half_col)]
        return remote(here, here, d2d_ss.at[h, g], d2d_rs.at[h, g], partner)

    def d2d_wait(h, g):
        d2d_all(h, g).wait_recv()

    def d2d_drain(g):
        for h in range(2):
            d2d_all(h, g).wait_send()

    def fill(h, g):
        p = parity(g)
        dest = ysend if h == 1 else mine

        @pl.when(core == 1)
        def _():
            for k in (1, 0):
                here = pl.ds(quarter - n_ovf, n_ovf)
                ovf_copy(h, g, 1 - k).wait_recv()
                dest[p, k, here] = dest[p, k, here] + ovf[h, p, k]
                if h == 1:
                    if g == 1 and k == 0:
                        y_copy(p, k, 0).start()
                    y_copy(p, k, 1).start()

    def ret_rows(p, k, i):
        start = (2 * p + k) * quarter + i * chunk
        return tok_peer.at[pl.ds(pl.multiple_of(start, chunk), chunk)]

    def ret_copy(p, k, i):
        d = p + 2 * k
        there = pl.ds(pl.multiple_of(i * region + ep * chunk, chunk), chunk)
        return remote(ret_rows(p, k, i), ret_recv.at[there], ret_ss, ret_rs.at[d, i], dev(d))

    def ret_wait(d, i):
        remote(tok_peer.at[pl.ds(0, chunk)], ret_recv.at[pl.ds(0, chunk)], ret_ss, ret_rs.at[d, i],
               peer).wait_recv()

    def reduce_chunk(g, k, i):
        p = parity(g)
        here = pl.ds(i * chunk, chunk)
        y_copy(p, k, i).wait_recv()
        total = (mine[p, k, here] + arrived[p, k, here]).astype(bf16)
        if k == 1:
            ret_rows(p, k, i)[...] = total
            ret_copy(p, k, i).start()
        else:
            @pl.when(p == 0)
            def _():
                ret_recv[pl.ds(pl.multiple_of(i * region + ep * chunk, chunk), chunk)] = total

            @pl.when(p == 1)
            def _():
                ret_rows(p, k, i)[...] = total
                ret_copy(p, k, i).start()

    out_rows = 256

    def combine(far, i, first=False):
        for d in ((2, 3) if far else (1,)):
            ret_wait(d, i)
        start = i * region + (lax.rem(col + far, 2)) * 2 * chunk
        here_r = pl.ds(pl.multiple_of(start, chunk), 2 * chunk)
        target = (iota((1, 2 * chunk), 1) + start).astype(f32)

        for j in range(n_tok // out_rows):
            here = pl.ds(j * out_rows, out_rows)
            pick = jnp.where(idx_col[here, :] == target, 1.0, 0.0).astype(bf16)
            got = jnp.dot(pick, ret_recv[here_r, :], preferred_element_type=f32)
            if first:
                out_ref[here, :] = got.astype(bf16)
            else:
                out_ref[here, :] = (out_ref[here, :].astype(f32) + got).astype(bf16)

    @pl.when(core == 0)
    def _():
        for cp in ytok[1:]:
            cp.wait_recv()
        dispatch(1, 2)

    def during_b(e):
        @pl.when(e == n_loc // 2)
        def _():
            fill(1, 0)

            @pl.when(core == 0)
            def _():
                ovf_start(0, 0)

    cnt_all = remote(cnts.at[pl.ds(1, 7)], cnts.at[pl.ds(1, 7)], cnt_ss, cnt_rs, peer)
    cnt_all.wait_recv()
    experts(0, lambda e: None)

    @pl.when(core == 1)
    def _():
        for e in range(n_loc // 2, n_loc):
            disp_start(0, e)
    compact(1, 0)

    @pl.when(core == 1)
    def _():
        for cp in ytok:
            cp.wait_recv()
        dispatch(1)
    compact(0, 0)
    pl.semaphore_signal(part_free, inc=1, device_id=partner, device_id_type=MESH)
    pl.semaphore_wait(part_free, 1)

    d2d_drain(0)
    experts(1, during_b)
    compact(1, 1)
    compact(0, 1)

    @pl.when(core == 0)
    def _():
        ovf_start(0, 1)
        for k, i in ((1, 0), (1, 1), (0, 0), (0, 1)):
            reduce_chunk(0, k, i)

    @pl.when(core == 1)
    def _():
        fill(0, 0)
        for k, i in ((1, 0), (0, 0), (1, 1)):
            reduce_chunk(0, k, i)
        fill(1, 1)
        reduce_chunk(0, 0, 1)

    ids_cp.wait_send()

    @pl.when(core == 1)
    def _():
        for cp in ytok:
            cp.wait_send()
    cnt_all.wait_send()

    for h in range(2):
        sent = send_rows.at[h, :, :, pl.ds(0, cap)]
        remote(sent, sent, disp_ss.at[h], disp_rs.at[0, 0], peer).wait_send()
    d2d_drain(1)

    @pl.when(core == 0)
    def _():
        reduce_chunk(1, 1, 0)
        reduce_chunk(1, 1, 1)
        combine(1, 0, True)
        combine(0, 0)
        combine(1, 1)
        combine(0, 1)
        reduce_chunk(1, 0, 0)
        reduce_chunk(1, 0, 1)

    @pl.when(core == 1)
    def _():
        reduce_chunk(1, 1, 0)
        fill(0, 1)
        combine(1, 0, True)
        reduce_chunk(1, 1, 1)
        reduce_chunk(1, 0, 0)
        combine(0, 0)
        combine(1, 1)
        reduce_chunk(1, 0, 1)
        combine(0, 1)

    @pl.when(core == 0)
    def _():
        for h in range(2):
            remote(ovf.at[h], ovf.at[h], ovf_ss.at[h], ovf_rs.at[0, 0, 0], peer).wait_send()
    for p in range(2):
        remote(ysend.at[p], ysend.at[p], y_ss.at[p], y_rs.at[0, 0, 0], peer).wait_send()
    ret_rest = tok_peer.at[pl.ds(quarter, 3 * quarter)]
    remote(ret_rest, ret_rest, ret_ss, ret_rs.at[0, 0], peer).wait_send()


def solution(mesh):
    n_ep, n_tp = mesh.shape['ep'], mesh.shape['tp']
    assert n_ep == 4 and n_tp == 2
    row_spec = P(('dp', 'ep', 'tp'), None)

    def local_moe(tokens, expert_ids, gate_vals, w_up, w_down):
        n_tok, hidden = tokens.shape
        n_loc, _, ffn = w_up.shape
        cap = capacity(n_tok, 1, n_loc * n_ep)
        pad = (cap + 15) // 16 * 16
        dims = (n_tok, hidden, ffn, n_loc, cap, pad)
        quarter = n_tok // 4
        col_slots = 2 * n_loc * cap
        n_ovf = col_slots - 2 * quarter
        f32, bf16 = jnp.float32, jnp.bfloat16
        dma = pltpu.SemaphoreType.DMA
        vmem = pl.BlockSpec(memory_space=pltpu.VMEM)
        hbm = pl.BlockSpec(memory_space=pl.ANY)
        picked = pl.pallas_call(
            functools.partial(moe_kernel, dims),
            out_shape=jax.ShapeDtypeStruct((n_tok, hidden), bf16),
            in_specs=[hbm, hbm, hbm, hbm],
            out_specs=vmem,
            scratch_shapes=[
                pltpu.VMEM((n_tok, hidden), bf16),
                pltpu.VMEM((n_tok, hidden), bf16),
                pltpu.VMEM((1, n_tok), jnp.int32),
                pltpu.VMEM((1, n_tok), jnp.int32),
                pltpu.VMEM((1, n_tok), f32),
                pltpu.VMEM((1, n_tok), f32),
                pltpu.VMEM((n_tok, 1), f32),
                pltpu.VMEM((8, 4 * n_loc, 128), f32),
                pltpu.VMEM((2, n_loc, 3, pad, hidden), bf16),
                pltpu.VMEM((2, n_loc, 4, pad, hidden), bf16),
                pltpu.VMEM((W_SLOTS, hidden, ffn), bf16),
                pltpu.VMEM((W_SLOTS, ffn, hidden), bf16),
                pltpu.VMEM((4 * pad, ffn), bf16),
                pltpu.VMEM((4, col_slots, hidden), f32),
                pltpu.VMEM((3 * col_slots, hidden), bf16),
                pltpu.VMEM((2, 2, quarter, hidden), f32),
                pltpu.VMEM((2, 2, quarter, hidden), f32),
                pltpu.VMEM((2, 2, quarter, hidden), f32),
                pltpu.VMEM((2, 2, 2, n_ovf, hidden), f32),
                pltpu.VMEM((n_tok, hidden), bf16),
                dma, dma, dma((W_SLOTS, 2, 2)), dma, dma, dma((3,)), dma((3,)), dma, dma,
                dma((2,)), dma((2, n_loc)), dma((2, 2)), dma((2, 2)), dma((2,)), dma((2, 2, 2)),
                dma((2,)), dma((2, 2, 2)), dma, dma((4, 2)),
                pltpu.SemaphoreType.REGULAR,
                pltpu.SemaphoreType.REGULAR,
            ],
            compiler_params=pltpu.CompilerParams(collective_id=0, has_side_effects=True, vmem_limit_bytes=VMEM_MIB << 20),
            name='moe_kernel',
        )(tokens, pltpu.with_memory_space_constraint(expert_ids.reshape(1, n_tok), pltpu.HBM), w_up, w_down)
        return (gate_vals * picked.astype(f32)).astype(bf16)

    return jax.shard_map(local_moe, mesh=mesh,
                         in_specs=(row_spec, row_spec, row_spec, P('ep', None, 'tp'), P('ep', 'tp', None)),
                         out_specs=row_spec, check_vma=False)
```
